32 devices in a mesh: shot: 2 (over y), inline: 4 (over z), xline: 2 (over x), depth: 2 (over core).
Axes of the slice: x: 2, y: 2, z: 4, core: 2. Of those that a mesh axis runs over, the one named last changes fastest.
Arguments:
- forward_now: float32 [2, 32, 64, 256], P(None, ('shot', 'inline'), 'xline', 'depth'), parts along dimension 1, may hold values from -6 to 6
- forward_before: float32 [2, 32, 64, 256], P(None, ('shot', 'inline'), 'xline', 'depth'), parts along dimension 1, may hold values from -6 to 6
- adjoint_now: float32 [2, 32, 64, 256], P(None, ('shot', 'inline'), 'xline', 'depth'), parts along dimension 1, may hold values from -6 to 6
- adjoint_before: float32 [2, 32, 64, 256], P(None, ('shot', 'inline'), 'xline', 'depth'), parts along dimension 1, may hold values from -6 to 6
- courant: float32 [16, 64, 256], P('inline', 'xline', 'depth'), may hold values from 0.04 to 0.15
- thomsen_epsilon: float32 [16, 64, 256], P('inline', 'xline', 'depth'), may hold values from 0.2 to 0.4
- thomsen_delta: float32 [16, 64, 256], P('inline', 'xline', 'depth'), may hold values from 0 to 0.2
- tilt_class: int32 [16, 64, 256], P('inline', 'xline', 'depth'), may hold values from 0 to 15
- azimuth_class: int32 [16, 64, 256], P('inline', 'xline', 'depth'), may hold values from 0 to 31
- tilt_table: float32 [16], replicated, may hold values from -3.140625 to 3.140625
- azimuth_table: float32 [32], replicated, may hold values from -3.140625 to 3.140625
- source_cell: int32 [2], P('shot'), parts along dimension 0, may hold values from 0 to 262143
- wavelet: float32 [8], P('shot'), parts along dimension 0, may hold values from -6 to 6
- receiver_cells: int32 [4096], P('shot'), parts along dimension 0, may hold values from 0 to 262143
- receiver_data: float32 [4, 4096], P(None, 'shot'), parts along dimension 1, may hold values from -6 to 6
Outputs:
- forward_fields: float32 [2, 32, 64, 256], P(None, ('shot', 'inline'), 'xline', 'depth'), parts along dimension 1
- adjoint_fields: float32 [2, 32, 64, 256], P(None, ('shot', 'inline'), 'xline', 'depth'), parts along dimension 1
- migrated_image: float32 [32, 64, 256], P(('shot', 'inline'), 'xline', 'depth'), parts along dimension 0
- traces: float32 [4, 4096], P(None, 'shot'), parts along dimension 1
The draws below stay inside these ranges and needn't reach their ends.
There are 2 independent parts, one for each index of `shot`. The reference program is written for one: setup_inputs(seed, part) draws one part's arguments, and reference() takes and returns one part's arrays. A program takes and returns all parts, laid end to end along the dimension named above; an argument that names none is the same for every part. Nothing has to cross between parts.
All inputs are finite; a program needn't handle non-finite values.
Results may differ from the reference program's by a relative error of at most 0.00002.
Values sent between devices are 32-bit elements; how exact they have to be, the bound alone decides.
A program may use at most 128 MiB of HBM per device.

```python
import jax
import jax.numpy as jnp

CX = 4
CY = 32
CZ = 128
STEPS = 4
NREC = 2048
NTILT = 16
NAZ = 32
NX = 16
NY = 64
NZ = 256


def draw_forward_now(key, part):
    array_shape = (2, NX, NY, NZ)
    values = jnp.clip(jax.random.normal(key, array_shape, jnp.float32), -6.0, 6.0)
    return values


def draw_receiver_cells(key, part):
    inline_blocks = NX // CX
    xline_blocks = NY // CY
    depth_blocks = NZ // CZ
    block_count = inline_blocks * xline_blocks * depth_blocks
    spread_count = NREC // 2
    block_shift = jax.random.randint(jax.random.fold_in(key, 10), (), 0, block_count, jnp.int32)
    spread_block = (jnp.arange(spread_count, dtype=jnp.int32) + block_shift) % block_count
    inline_block = spread_block // (xline_blocks * depth_blocks)
    xline_block = spread_block // depth_blocks % xline_blocks
    depth_block = spread_block % depth_blocks
    inline_local = jax.random.randint(jax.random.fold_in(key, 11), (spread_count,), 0, CX, jnp.int32)
    xline_local = jax.random.randint(jax.random.fold_in(key, 12), (spread_count,), 0, CY, jnp.int32)
    depth_local = jax.random.randint(jax.random.fold_in(key, 13), (spread_count,), 0, CZ, jnp.int32)
    spread_cells = ((inline_block * CX + inline_local) * NY + xline_block * CY + xline_local) * NZ + depth_block * CZ + depth_local
    loose_count = NREC - spread_count
    loose_inline = jax.random.randint(jax.random.fold_in(key, 14), (loose_count,), 0, NX, jnp.int32)
    loose_xline = jax.random.randint(jax.random.fold_in(key, 15), (loose_count,), 0, NY, jnp.int32)
    loose_depth = jax.random.randint(jax.random.fold_in(key, 16), (loose_count,), 0, NZ, jnp.int32)
    loose_cells = (loose_inline * NY + loose_xline) * NZ + loose_depth
    every_cell = jnp.concatenate([spread_cells, loose_cells]).astype(jnp.int32)
    order = jax.random.permutation(jax.random.fold_in(key, 17), NREC)
    return every_cell[order].astype(jnp.int32)


def set_ends(array, own_key, smallest, largest):
    shape = array.shape
    index_at = [jax.random.randint(jax.random.fold_in(own_key, axis), (), 0, shape[axis]) for axis in range(len(shape))]
    array = array.at[tuple(index_at)].set(smallest)
    longest = shape.index(max(shape))
    index_at[longest] = (index_at[longest] + 1) % shape[longest]
    return array.at[tuple(index_at)].set(largest)


def level_of(rng, extent, shards, smallest, top_value):
    level, own = 1.0, jax.random.fold_in(rng, 6)
    for dim, parts in shards:
        heights = jnp.exp(jax.random.uniform(jax.random.fold_in(own, dim), (parts,), jnp.float32, smallest / len(shards), top_value / len(shards)))
        level = level * jnp.repeat(heights, extent[dim] // parts).reshape([-1 if axis == dim else 1 for axis in range(len(extent))])
    return level


def bell_draw(stream_key, shape, scale, limit, shards=(), kind=jnp.bfloat16):
    entries = jax.random.normal(stream_key, shape, jnp.float32) * scale
    if len(shards) > 0:
        entries = level_of(stream_key, shape, shards, -0.22, 0.18) * entries
    return jnp.clip(entries, min=-limit, max=limit).astype(kind)


def setup_inputs(seed: int = 0, part: int = 0) -> dict:
    streams_of = jax.random.split(jax.random.key(seed), 16)
    own_keys = jax.random.split(jax.random.fold_in(streams_of[15], part), 16)
    forward_now = draw_forward_now(jax.random.fold_in(jax.random.fold_in(streams_of[15], part), 71), part)
    forward_before = bell_draw(own_keys[1], (2, NX, NY, NZ), 1.0, 6.0, ((1, 4), (2, 2), (3, 2)), jnp.float32)
    adjoint_now = bell_draw(own_keys[2], (2, NX, NY, NZ), 1.0, 6.0, ((1, 4), (2, 2), (3, 2)), jnp.float32)
    adjoint_before = bell_draw(own_keys[3], (2, NX, NY, NZ), 1.0, 6.0, ((1, 4), (2, 2), (3, 2)), jnp.float32)
    courant = jnp.clip(0.04 + 0.11000001 * jax.random.uniform(streams_of[4], (NX, NY, NZ), jnp.float32) ** level_of(streams_of[4], (NX, NY, NZ), ((0, 4), (1, 2), (2, 2)), -0.2, 0.2), 0.04, 0.15)
    thomsen_epsilon = jnp.clip(0.2 + 0.2 * jax.random.uniform(streams_of[5], (NX, NY, NZ), jnp.float32) ** level_of(streams_of[5], (NX, NY, NZ), ((0, 4), (1, 2), (2, 2)), -0.2, 0.2), 0.2, 0.4)
    thomsen_delta = jnp.clip(0.2 * jax.random.uniform(streams_of[6], (NX, NY, NZ), jnp.float32) ** level_of(streams_of[6], (NX, NY, NZ), ((0, 4), (1, 2), (2, 2)), -0.2, 0.2), 0.0, 0.2)
    tilt_class = set_ends(jax.random.randint(streams_of[7], (NX, NY, NZ), 0, NTILT), jax.random.fold_in(streams_of[7], 1), 0, NTILT - 1).astype(jnp.int32)
    azimuth_class = set_ends(jax.random.randint(streams_of[8], (NX, NY, NZ), 0, NAZ), jax.random.fold_in(streams_of[8], 1), 0, NAZ - 1).astype(jnp.int32)
    tilt_table = jnp.clip(jax.random.uniform(streams_of[9], (NTILT,), jnp.float32, -3.140625, 3.140625), -3.140625, 3.140625)
    azimuth_table = jnp.clip(jax.random.uniform(streams_of[10], (NAZ,), jnp.float32, -3.140625, 3.140625), -3.140625, 3.140625)
    source_cell = jax.random.randint(own_keys[11], (1,), 0, NX * NY * NZ).astype(jnp.int32)
    wavelet = bell_draw(own_keys[12], (STEPS,), 1.0, 6.0, (), jnp.float32)
    receiver_cells = draw_receiver_cells(jax.random.fold_in(jax.random.fold_in(streams_of[15], part), 71), part)
    receiver_data = bell_draw(own_keys[14], (STEPS, NREC), 1.0, 6.0, (), jnp.float32)
    return dict(forward_now=forward_now, forward_before=forward_before, adjoint_now=adjoint_now, adjoint_before=adjoint_before, courant=courant, thomsen_epsilon=thomsen_epsilon, thomsen_delta=thomsen_delta, tilt_class=tilt_class, azimuth_class=azimuth_class, tilt_table=tilt_table, azimuth_table=azimuth_table, source_cell=source_cell, wavelet=wavelet, receiver_cells=receiver_cells, receiver_data=receiver_data)


def differences(padded):
    centre = padded[..., 1:-1, 1:-1, 1:-1]
    inline_inline = padded[..., 2:, 1:-1, 1:-1] + padded[..., :-2, 1:-1, 1:-1] - 2.0 * centre
    xline_xline = padded[..., 1:-1, 2:, 1:-1] + padded[..., 1:-1, :-2, 1:-1] - 2.0 * centre
    depth_depth = padded[..., 1:-1, 1:-1, 2:] + padded[..., 1:-1, 1:-1, :-2] - 2.0 * centre
    inline_xline = 0.25 * (padded[..., 2:, 2:, 1:-1] - padded[..., 2:, :-2, 1:-1] - padded[..., :-2, 2:, 1:-1] + padded[..., :-2, :-2, 1:-1])
    inline_depth = 0.25 * (padded[..., 2:, 1:-1, 2:] - padded[..., 2:, 1:-1, :-2] - padded[..., :-2, 1:-1, 2:] + padded[..., :-2, 1:-1, :-2])
    xline_depth = 0.25 * (padded[..., 1:-1, 2:, 2:] - padded[..., 1:-1, 2:, :-2] - padded[..., 1:-1, :-2, 2:] + padded[..., 1:-1, :-2, :-2])
    return centre, inline_inline, xline_xline, depth_depth, inline_xline, inline_depth, xline_depth


def advance_pair(padded, before, factors):
    centre, inline_inline, xline_xline, depth_depth, inline_xline, inline_depth, xline_depth = differences(padded)
    axial_part = (factors[3] * inline_inline + factors[4] * xline_xline + factors[5] * depth_depth
                  + factors[6] * inline_xline + factors[7] * inline_depth + factors[8] * xline_depth)
    plane_part = (inline_inline + xline_xline + depth_depth)[0] - axial_part[0]
    pressure = 2.0 * centre[0] - before[0] + factors[0] * plane_part + factors[2] * axial_part[1]
    auxiliary = 2.0 * centre[1] - before[1] + factors[1] * plane_part + factors[2] * axial_part[1]
    return jnp.stack([pressure, auxiliary])


def coefficients(courant, thomsen_epsilon, thomsen_delta, tilt_sine, tilt_cosine, azimuth_cosine, azimuth_sine):
    axis_first = tilt_sine * azimuth_cosine
    axis_second = tilt_sine * azimuth_sine
    axis_third = tilt_cosine
    return jnp.stack([courant * (1.0 + 2.0 * thomsen_epsilon), courant * (1.0 + 2.0 * thomsen_delta), courant,
                      axis_first * axis_first, axis_second * axis_second, axis_third * axis_third,
                      2.0 * axis_first * axis_second, 2.0 * axis_first * axis_third, 2.0 * axis_second * axis_third])


def reference(forward_now, forward_before, adjoint_now, adjoint_before, courant, thomsen_epsilon, thomsen_delta,
              tilt_class, azimuth_class, tilt_table, azimuth_table, source_cell, wavelet, receiver_cells, receiver_data):
    tilt_sine = jnp.sin(tilt_table)[tilt_class]
    tilt_cosine = jnp.cos(tilt_table)[tilt_class]
    azimuth_cosine = jnp.cos(azimuth_table)[azimuth_class]
    azimuth_sine = jnp.sin(azimuth_table)[azimuth_class]
    factors = coefficients(courant, thomsen_epsilon, thomsen_delta, tilt_sine, tilt_cosine, azimuth_cosine, azimuth_sine)
    forward_current, forward_previous = forward_now, forward_before
    adjoint_current, adjoint_previous = adjoint_now, adjoint_before
    volume = NX * NY * NZ
    padding = ((0, 0), (1, 1), (1, 1), (1, 1))
    image_sum = jnp.zeros((NX, NY, NZ), jnp.float32)
    records = []
    for moment in range(STEPS):
        forward_next = advance_pair(jnp.pad(forward_current, padding), forward_previous, factors)
        adjoint_next = advance_pair(jnp.pad(adjoint_current, padding), adjoint_previous, factors)
        source_term = jnp.zeros((volume,), jnp.float32).at[source_cell].add(
            jnp.broadcast_to(wavelet[moment], source_cell.shape)).reshape(NX, NY, NZ)
        receiver_term = jnp.zeros((volume,), jnp.float32).at[receiver_cells].add(
            receiver_data[moment]).reshape(NX, NY, NZ)
        forward_next = forward_next + source_term[None]
        adjoint_next = adjoint_next + receiver_term[None]
        records.append(forward_next[0].reshape(volume)[receiver_cells])
        image_sum = image_sum + forward_next[0] * adjoint_next[0] + forward_next[1] * adjoint_next[1]
        forward_previous, forward_current = forward_current, forward_next
        adjoint_previous, adjoint_current = adjoint_current, adjoint_next
    return forward_current, adjoint_current, image_sum, jnp.stack(records)
```

```python
import functools

import jax
import jax.numpy as jnp
from jax import lax
from jax.experimental import pallas as pl
from jax.experimental.pallas import tpu as pltpu
from jax.sharding import PartitionSpec as P

STEPS = 4
MESH = pl.DeviceIdType.MESH
AXES = ("inline", "xline", "depth")
LANES = 128
TOP = 8

DIRECTIONS = [(a, b) for a in (-1, 0, 1) for b in (-1, 0, 1) if (a, b) != (0, 0)]
SIDES = [d for d in DIRECTIONS if d[0] == 0]
FACES = [d for d in DIRECTIONS if d[0] != 0]


def split_by(values, size):
    if size & (size - 1) == 0:
        return values >> (size.bit_length() - 1), values & (size - 1)
    quotient = lax.div(values, jnp.int32(size))
    return quotient, values - quotient * size


def three_parts(values):
    high = values.astype(jnp.bfloat16).astype(jnp.float32)
    rest = values - high
    middle = rest.astype(jnp.bfloat16).astype(jnp.float32)
    return high, middle, rest - middle


def kernel(
    sizes,
    forward_now,
    forward_before,
    adjoint_now,
    adjoint_before,
    courant,
    epsilon,
    delta,
    tilt_class,
    azimuth_class,
    tilt_table,
    azimuth_table,
    source_cell,
    wavelet,
    receiver_cells,
    receiver_data,
    forward_out,
    adjoint_out,
    image_out,
    traces_out,
    fields,
    model,
    classes,
    factors,
    zdiff,
    zsum,
    image,
    hot_row,
    hot_lane,
    spread,
    terms,
    trace_own,
    trace_got,
    trace_all,
    load_sem,
    ship_send,
    ship_recv,
    first_send,
    first_recv,
    halo_send,
    halo_recv,
    trace_send,
    trace_recv,
    result_send,
    result_recv,
):
    n_in, n_x, n_d = sizes
    _, cx, cy, cz = forward_now.shape
    nrec = receiver_cells.shape[1]
    groups = cy // 8
    here = tuple(lax.axis_index(axis) for axis in AXES)
    rows = slice(TOP, TOP + cy)
    up = slice(TOP - 1, TOP + cy - 1)
    down = slice(TOP + 1, TOP + cy + 1)
    top = n_d - 1
    leader = here[2] == top
    nows = (forward_now, adjoint_now)

    def present(direction):
        ok = None
        for at, step, size in zip(here, direction, sizes):
            if step == 0:
                continue
            this = (at < size - 1) if step > 0 else (at > 0)
            ok = this if ok is None else jnp.logical_and(ok, this)
        return ok

    def target(direction, depth):
        place = {axis: at + step for axis, at, step in zip(AXES, here, direction) if step != 0}
        return {**place, "depth": depth}

    def opposite(d):
        return tuple(-step for step in d)

    live = [d for d in DIRECTIONS if all(s == 0 or n > 1 for s, n in zip(d, sizes))]
    peers = [(a, b) for a in range(n_in) for b in range(n_x) if (a, b) != (0, 0)]

    def peer(k):
        return {
            "inline": lax.rem(here[0] + peers[k][0], n_in),
            "xline": lax.rem(here[1] + peers[k][1], n_x),
        }

    def at_depth(depth):
        return {"depth": depth}

    inputs = [
        (forward_now, lambda t: fields.at[1, 0, :, pl.ds(1, cx), t, pl.ds(TOP, cy)]),
        (courant, lambda t: model.at[0, :, t]),
        (epsilon, lambda t: model.at[1, :, t]),
        (delta, lambda t: model.at[2, :, t]),
        (tilt_class, lambda t: classes.at[0, :, t]),
        (azimuth_class, lambda t: classes.at[1, :, t]),
        (forward_before, lambda t: fields.at[0, 0, :, pl.ds(1, cx), t, pl.ds(TOP, cy)]),
        (adjoint_now, lambda t: fields.at[1, 1, :, pl.ds(1, cx), t, pl.ds(TOP, cy)]),
        (adjoint_before, lambda t: fields.at[0, 1, :, pl.ds(1, cx), t, pl.ds(TOP, cy)]),
    ]

    def load(number):
        source, place = inputs[number]
        return pltpu.make_async_copy(source, place(top), load_sem.at[number])

    def ship(number, t):
        source, place = inputs[number]
        return pltpu.make_async_remote_copy(
            src_ref=source,
            dst_ref=place(t),
            send_sem=ship_send.at[number],
            recv_sem=ship_recv.at[t, number],
            device_id=at_depth(top),
            device_id_type=MESH,
        )

    def wait_input(number):
        load(number).wait()
        for t in range(top):
            ship(number, t).wait_recv()

    def edge(step, size, first):
        if step == 0:
            return pl.ds(first, size)
        return pl.ds(first + size - 1 if step > 0 else first, 1)

    def beyond(step, size, first):
        if step == 0:
            return pl.ds(first, size)
        return pl.ds(first - 1 if step > 0 else first + size, 1)

    def first_copy(d, system, t):
        return pltpu.make_async_remote_copy(
            src_ref=nows[system].at[:, edge(d[0], cx, 0), edge(d[1], cy, 0)],
            dst_ref=fields.at[1, system, :, beyond(d[0], cx, 1), t, beyond(d[1], cy, TOP)],
            send_sem=first_send.at[system, DIRECTIONS.index(d)],
            recv_sem=first_recv.at[t, system, DIRECTIONS.index(d)],
            device_id=target(d, top),
            device_id_type=MESH,
        )

    def halo_copy(d, s, system):
        return pltpu.make_async_remote_copy(
            src_ref=fields.at[s + 1, system, :, edge(d[0], cx, 1), :, edge(d[1], cy, TOP)],
            dst_ref=fields.at[s + 1, system, :, beyond(d[0], cx, 1), :, beyond(d[1], cy, TOP)],
            send_sem=halo_send.at[s, system, DIRECTIONS.index(d)],
            recv_sem=halo_recv.at[s, system, DIRECTIONS.index(d)],
            device_id=target(d, top),
            device_id_type=MESH,
        )

    def trace_copy(s, k):
        return pltpu.make_async_remote_copy(
            src_ref=trace_own.at[s],
            dst_ref=trace_got.at[s, k],
            send_sem=trace_send.at[s, k],
            recv_sem=trace_recv.at[s, k],
            device_id=peer(k),
            device_id_type=MESH,
        )

    results = [
        (lambda t: fields.at[STEPS + 1, 0, :, pl.ds(1, cx), t, pl.ds(TOP, cy)], forward_out),
        (lambda t: fields.at[STEPS + 1, 1, :, pl.ds(1, cx), t, pl.ds(TOP, cy)], adjoint_out),
        (lambda t: image.at[t], image_out),
        (lambda t: trace_all, traces_out),
    ]

    def result_copy(number, t):
        source, place = results[number]
        return pltpu.make_async_remote_copy(
            src_ref=source(t),
            dst_ref=place,
            send_sem=result_send.at[number, t],
            recv_sem=result_recv.at[number],
            device_id=at_depth(t),
            device_id_type=MESH,
        )

    def give_result(number):
        for t in range(top):
            result_copy(number, t).start()

    barrier = pltpu.get_barrier_semaphore()

    def greet(place):
        pl.semaphore_signal(barrier, inc=1, device_id=place, device_id_type=MESH)

    def send_first(t):
        for system in range(2):
            for d in sorted(live, key=lambda d: d[0] == 0):

                @pl.when(present(d))
                def _(d=d):
                    first_copy(d, system, t).start()

    def drain_first(t):
        for system in range(2):
            for d in live:

                @pl.when(present(d))
                def _(d=d):
                    first_copy(d, system, t).wait_send()

    def clear(d):
        for s in range(STEPS):
            for system in range(2):
                place = fields.at[
                    s + 1, system, :, beyond(d[0], cx, 1), :, beyond(d[1], cy, TOP)
                ]
                place[...] = jnp.zeros(place.shape, jnp.float32)

    def clear_absent():
        for d in DIRECTIONS:
            if d not in live:
                clear(d)
            else:

                @pl.when(jnp.logical_not(present(opposite(d))))
                def _(d=d):
                    clear(d)

    def send(s, system, which):
        for d in which:
            if d in live:

                @pl.when(present(d))
                def _(d=d):
                    halo_copy(d, s, system).start()

    def receive(s, system, which):
        for d in which:
            if d in live:

                @pl.when(present(opposite(d)))
                def _(d=d):
                    if s == 0:
                        for t in range(n_d):
                            first_copy(d, system, t).wait_recv()
                    else:
                        halo_copy(d, s, system).wait_recv()

    def drain(s, system):
        for d in live:

            @pl.when(present(d))
            def _(d=d):
                halo_copy(d, s, system).wait_send()

    lane = lax.broadcasted_iota(jnp.int32, (8, LANES), 1)
    first_lane, last_lane = lane == 0, lane == LANES - 1

    def along_depth(s, system, f, plane, row):
        tiles = [fields[s + 1, system, f, plane, t, row : row + 8, :] for t in range(n_d)]
        right = [pltpu.roll(tile, 1, 1) for tile in tiles]
        left = [pltpu.roll(tile, LANES - 1, 1) for tile in tiles]
        before = [
            jnp.where(first_lane, right[t - 1] if t > 0 else 0.0, right[t]) for t in range(n_d)
        ]
        after = [
            jnp.where(last_lane, left[t + 1] if t < top else 0.0, left[t]) for t in range(n_d)
        ]
        return before, after

    def own_depth(s, system):
        for f in range(2):
            for i in range(cx):
                for r in range(groups):
                    before, after = along_depth(s, system, f, i + 1, TOP + 8 * r)
                    for t in range(n_d):
                        at = slice(TOP + 8 * r, TOP + 8 * r + 8)
                        zdiff[system, f, i + 1, t, at, :] = after[t] - before[t]
                        zsum[system, f, i, t, 8 * r : 8 * r + 8, :] = after[t] + before[t]

    def side_depth(s, system):
        for f in range(2):
            for i in range(cx):
                for row in (0, TOP + cy):
                    before, after = along_depth(s, system, f, i + 1, row)
                    for t in range(n_d):
                        zdiff[system, f, i + 1, t, row : row + 8, :] = after[t] - before[t]

    def face_depth(s, system, plane):
        for f in range(2):
            for r in range(groups):
                before, after = along_depth(s, system, f, plane, TOP + 8 * r)
                for t in range(n_d):
                    at = slice(TOP + 8 * r, TOP + 8 * r + 8)
                    zdiff[system, f, plane, t, at, :] = after[t] - before[t]

    outer = sorted({0, cx - 1})
    inner = [i for i in range(cx) if i not in outer]

    def advance(s, system, i):
        for t in range(n_d):
            axial = []
            lap = None
            doubled = []
            for f in range(2):
                now = fields.at[s + 1, system, f]
                slope = zdiff.at[system, f]
                twice = 2.0 * now[i + 1, t, rows, :]
                doubled.append(twice)
                dxx = now[i + 2, t, rows, :] + now[i, t, rows, :] - twice
                dyy = now[i + 1, t, down, :] + now[i + 1, t, up, :] - twice
                dzz = zsum[system, f, i, t] - twice
                dxy = (
                    now[i + 2, t, down, :]
                    - now[i + 2, t, up, :]
                    - now[i, t, down, :]
                    + now[i, t, up, :]
                )
                dxz = slope[i + 2, t, rows, :] - slope[i, t, rows, :]
                dyz = slope[i + 1, t, down, :] - slope[i + 1, t, up, :]
                axial.append(
                    factors[3, i, t] * dxx
                    + factors[4, i, t] * dyy
                    + factors[5, i, t] * dzz
                    + factors[6, i, t] * dxy
                    + factors[7, i, t] * dxz
                    + factors[8, i, t] * dyz
                )
                if f == 0:
                    lap = dxx + dyy + dzz
            plane_part = lap - axial[0]
            along = factors[2, i, t] * axial[1]
            if system == 0:
                row_at = lax.broadcasted_iota(jnp.int32, (cy, LANES), 0)
                lane_at = lax.broadcasted_iota(jnp.int32, (cy, LANES), 1)
                cell = (
                    (here[0] * cx + i) * (n_x * cy) + here[1] * cy + row_at
                ) * (n_d * cz) + t * cz + lane_at
                added = jnp.where(cell == source_cell[0], wavelet[s], 0.0)
            else:
                added = terms[s, i, t]
            new = []
            for f in range(2):
                value = (
                    doubled[f]
                    - fields[s, system, f, i + 1, t, rows, :]
                    + factors[f, i, t] * plane_part
                    + along
                    + added
                )
                fields[s + 2, system, f, i + 1, t, rows, :] = value
                new.append(value)
            if system == 1:
                product = (
                    fields[s + 2, 0, 0, i + 1, t, rows, :] * new[0]
                    + fields[s + 2, 0, 1, i + 1, t, rows, :] * new[1]
                )
                if s > 0:
                    product = image[t, i] + product
                if s == STEPS - 1 and t == top:
                    image_out[i] = product
                else:
                    image[t, i] = product
            if s == STEPS - 1 and t == top:
                out = forward_out if system == 0 else adjoint_out
                out[0, i] = new[0]
                out[1, i] = new[1]

    def coefficients():
        tilt_sine, tilt_cosine = jnp.sin(tilt_table[...]), jnp.cos(tilt_table[...])
        turn_sine, turn_cosine = jnp.sin(azimuth_table[...]), jnp.cos(azimuth_table[...])

        def look(which, i, t, tables):
            chosen = classes[which, i, t]
            found = [jnp.zeros((cy, LANES), jnp.float32) for _ in tables]
            for k in range(tables[0].shape[1]):
                match = chosen == k
                found = [
                    jnp.where(match, jnp.broadcast_to(v[:, k : k + 1], (cy, LANES)), w)
                    for v, w in zip(tables, found)
                ]
            return found

        for i in range(cx):
            for t in range(n_d):
                sine, third = look(0, i, t, (tilt_sine, tilt_cosine))
                turned, across = look(1, i, t, (turn_cosine, turn_sine))
                first, second = sine * turned, sine * across
                base = model[0, i, t]
                factors[0, i, t] = base * (1.0 + 2.0 * model[1, i, t])
                factors[1, i, t] = base * (1.0 + 2.0 * model[2, i, t])
                factors[2, i, t] = base
                factors[3, i, t] = first * first
                factors[4, i, t] = second * second
                factors[5, i, t] = third * third
                factors[6, i, t] = 0.5 * first * second
                factors[7, i, t] = 0.5 * first * third
                factors[8, i, t] = 0.5 * second * third

    volume = cx * cy
    wide = n_d * cz

    def receivers():
        cells = receiver_cells[...]
        upper, depth_at = split_by(cells, wide)
        inline_at, xline_at = split_by(upper, n_x * cy)
        inline_at = inline_at - here[0] * cx
        xline_at = xline_at - here[1] * cy
        inside = (inline_at >= 0) & (inline_at < cx) & (xline_at >= 0) & (xline_at < cy)
        row_of = jnp.where(inside, inline_at * cy + xline_at, -1)
        row_match = (
            lax.broadcasted_iota(jnp.int32, (volume, nrec), 0)
            == jnp.broadcast_to(row_of, (volume, nrec))
        )
        lane_match = (
            lax.broadcasted_iota(jnp.int32, (wide, nrec), 0)
            == jnp.broadcast_to(depth_at, (wide, nrec))
        )
        hot_row[...] = jnp.where(row_match, 1.0, 0.0)
        lanes_hot = jnp.where(lane_match, 1.0, 0.0).astype(jnp.bfloat16)
        for part in range(3):
            hot_lane[part * wide : (part + 1) * wide, :] = lanes_hot
        parts = three_parts(receiver_data[...])
        for s in range(STEPS):
            for number, part in enumerate(parts):
                start = (s * 3 + number) * volume
                spread[start : start + volume, :] = (
                    hot_row[...] * jnp.broadcast_to(part[s : s + 1, :], (volume, nrec))
                ).astype(jnp.bfloat16)
            got = lax.dot_general(
                spread[s * 3 * volume : (s + 1) * 3 * volume, :],
                hot_lane[0:wide, :],
                (((1,), (1,)), ((), ())),
                preferred_element_type=jnp.float32,
            )
            total = got[:volume] + got[volume : 2 * volume] + got[2 * volume :]
            for i in range(cx):
                for t in range(n_d):
                    terms[s, i, t] = total[i * cy : (i + 1) * cy, t * cz : (t + 1) * cz]

    def sample(s):
        tiles = [
            jnp.concatenate(
                [fields[s + 2, 0, 0, i + 1, t, rows, :] for i in range(cx)], axis=0
            )
            for t in range(n_d)
        ]
        split = [three_parts(tile) for tile in tiles]
        parts = jnp.concatenate(
            [split[t][part].astype(jnp.bfloat16) for part in range(3) for t in range(n_d)],
            axis=1,
        )
        picked = jnp.dot(parts, hot_lane[...], preferred_element_type=jnp.float32)
        trace_own[s] = jnp.sum(picked * hot_row[...], axis=0, keepdims=True)

    def share(s):
        for k in range(len(peers)):
            trace_copy(s, k).start()

    def finish_trace(s):
        total = trace_own[s]
        for k in range(len(peers)):
            trace_copy(s, k).wait_recv()
            total = total + trace_got[s, k]
        traces_out[s : s + 1, :] = total
        trace_all[s : s + 1, :] = total

    @pl.when(jnp.logical_not(leader))
    def _():
        greet(at_depth(top))
        expected = jnp.int32(1)
        for d in live:
            expected = expected + jnp.where(present(d), 1, 0)
        pl.semaphore_wait(barrier, expected)
        send_first(here[2])
        for number in range(len(inputs)):
            ship(number, here[2]).start()
        for number in range(len(inputs)):
            ship(number, here[2]).wait_send()
        drain_first(here[2])
        for number in range(len(results)):
            result_copy(number, here[2]).wait_recv()

    @pl.when(leader)
    def _():
        for number in range(len(inputs)):
            load(number).start()
        for t in range(top):
            greet(at_depth(t))
        for k in range(len(peers)):
            greet(peer(k))
        for d in live:

            @pl.when(present(d))
            def _(d=d):
                for t in range(top):
                    greet(target(d, t))

        pl.semaphore_wait(barrier, len(peers) + top)
        send_first(top)
        clear_absent()
        receivers()
        for number in range(1, 6):
            wait_input(number)
        coefficients()
        wait_input(0)
        own_depth(0, 0)
        wait_input(6)
        for s in range(STEPS):
            for system in range(2):
                if s == 0 and system == 1:
                    wait_input(7)
                    own_depth(0, 1)
                    wait_input(8)
                receive(s, system, SIDES)
                side_depth(s, system)
                for i in inner:
                    advance(s, system, i)
                receive(s, system, FACES)
                for plane in (0, cx + 1):
                    face_depth(s, system, plane)
                for i in outer:
                    advance(s, system, i)
                    if s < STEPS - 1:
                        if i == 0:
                            send(s + 1, system, [d for d in FACES if d[0] < 0])
                        if i == cx - 1:
                            send(s + 1, system, [d for d in FACES if d[0] > 0])
                if s < STEPS - 1:
                    send(s + 1, system, SIDES)
                    own_depth(s + 1, system)
                else:
                    give_result(system)
                    if system == 0:
                        sample(s)
                        share(s)
            if s < STEPS - 1:
                sample(s)
                share(s)
        give_result(2)
        for s in range(STEPS):
            finish_trace(s)
        give_result(3)
        drain_first(top)
        for s in range(1, STEPS):
            for system in range(2):
                drain(s, system)
        for s in range(STEPS):
            for k in range(len(peers)):
                trace_copy(s, k).wait_send()
        for number in range(len(results)):
            for t in range(top):
                result_copy(number, t).wait_send()


def publish(*refs):
    half = len(refs) // 2
    for source, place in zip(refs[:half], refs[half:]):
        place[...] = source[...]


def per_device(sizes, *operands):
    shapes = [operand.shape for operand in operands]
    _, cx, cy, cz = shapes[0]
    nrec = shapes[13][0]
    n_in, n_x, n_d = sizes
    operands = list(operands)
    for which in (9, 10, 13):
        operands[which] = operands[which].reshape(1, -1)
    f32, bf16 = jnp.float32, jnp.bfloat16
    padded = cy + 2 * TOP
    chips = n_in * n_x
    count = len(DIRECTIONS)
    dma = pltpu.SemaphoreType.DMA
    scratch = [
        pltpu.VMEM((STEPS + 2, 2, 2, cx + 2, n_d, padded, cz), f32),
        pltpu.VMEM((3, cx, n_d, cy, cz), f32),
        pltpu.VMEM((2, cx, n_d, cy, cz), jnp.int32),
        pltpu.VMEM((9, cx, n_d, cy, cz), f32),
        pltpu.VMEM((2, 2, cx + 2, n_d, padded, cz), f32),
        pltpu.VMEM((2, 2, cx, n_d, cy, cz), f32),
        pltpu.VMEM((n_d, cx, cy, cz), f32),
        pltpu.VMEM((cx * cy, nrec), f32),
        pltpu.VMEM((3 * n_d * cz, nrec), bf16),
        pltpu.VMEM((3 * STEPS * cx * cy, nrec), bf16),
        pltpu.VMEM((STEPS, cx, n_d, cy, cz), f32),
        pltpu.VMEM((STEPS, 1, nrec), f32),
        pltpu.VMEM((STEPS, chips, 1, nrec), f32),
        pltpu.VMEM((STEPS, nrec), f32),
        dma((9,)),
        dma((9,)),
        dma((n_d, 9)),
        dma((2, count)),
        dma((n_d, 2, count)),
        dma((STEPS, 2, count)),
        dma((STEPS, 2, count)),
        dma((STEPS, chips)),
        dma((STEPS, chips)),
        dma((4, n_d)),
        dma((4,)),
    ]
    vmem = pl.BlockSpec(memory_space=pltpu.VMEM)
    smem = pl.BlockSpec(memory_space=pltpu.SMEM)
    anywhere = pl.BlockSpec(memory_space=pl.ANY)
    made = pl.pallas_call(
        functools.partial(kernel, sizes),
        out_shape=(
            jax.ShapeDtypeStruct((2, cx, cy, cz), f32),
            jax.ShapeDtypeStruct((2, cx, cy, cz), f32),
            jax.ShapeDtypeStruct((cx, cy, cz), f32),
            jax.ShapeDtypeStruct((STEPS, nrec), f32),
        ),
        in_specs=[anywhere] * 9 + [vmem, vmem, smem, smem, vmem, vmem],
        out_specs=(vmem, vmem, vmem, vmem),
        scratch_shapes=scratch,
        compiler_params=pltpu.CompilerParams(
            collective_id=0, has_side_effects=True, vmem_limit_bytes=56 * 2**20
        ),
        name="wavefields",
    )(*operands)
    return pl.pallas_call(
        publish,
        out_shape=[jax.ShapeDtypeStruct(m.shape, m.dtype) for m in made],
        in_specs=[vmem] * len(made),
        out_specs=[vmem] * len(made),
        name="publish",
    )(*made)


def solution(mesh):
    sizes = tuple(mesh.shape[axis] for axis in AXES)
    field = P(None, ("shot", "inline"), "xline", "depth")
    cell = P("inline", "xline", "depth")
    return jax.shard_map(
        functools.partial(per_device, sizes),
        mesh=mesh,
        in_specs=(
            field, field, field, field,
            cell, cell, cell, cell, cell,
            P(), P(), P("shot"), P("shot"), P("shot"), P(None, "shot"),
        ),
        out_specs=(field, field, P(("shot", "inline"), "xline", "depth"), P(None, "shot")),
        check_vma=False,
    )
```

```python
import functools

import jax
import jax.numpy as jnp
from jax import lax
from jax.experimental import pallas as pl
from jax.experimental.pallas import tpu as pltpu
from jax.sharding import PartitionSpec as P

STEPS = 4
MESH = pl.DeviceIdType.MESH
AXES = ("inline", "xline", "depth")
LANES = 128
TOP = 8

DIRECTIONS = [(a, b) for a in (-1, 0, 1) for b in (-1, 0, 1) if (a, b) != (0, 0)]
SIDES = [d for d in DIRECTIONS if d[0] == 0]
FACES = [d for d in DIRECTIONS if d[0] != 0]


def split_by(values, size):
    if size & (size - 1) == 0:
        return values >> (size.bit_length() - 1), values & (size - 1)
    quotient = lax.div(values, jnp.int32(size))
    return quotient, values - quotient * size


def two_parts(values):
    high = values.astype(jnp.bfloat16)
    return high, (values - high.astype(jnp.float32)).astype(jnp.bfloat16)


def kernel(
    sizes,
    forward_now,
    forward_before,
    adjoint_now,
    adjoint_before,
    courant,
    epsilon,
    delta,
    tilt_class,
    azimuth_class,
    tilt_given,
    azimuth_given,
    source_given,
    wavelet_given,
    cells_given,
    data_given,
    forward_out,
    adjoint_out,
    image_out,
    traces_out,
    fields,
    model,
    classes,
    factors,
    zdiff,
    zsum,
    image,
    tilt_table,
    azimuth_table,
    source_cell,
    wavelet,
    receiver_cells,
    receiver_data,
    hot_row,
    hot_lane,
    spread,
    terms,
    trace_own,
    trace_got,
    trace_all,
    load_sem,
    small_sem,
    ship_send,
    ship_recv,
    first_send,
    first_recv,
    halo_send,
    halo_recv,
    trace_send,
    trace_recv,
    result_send,
    result_recv,
):
    n_in, n_x, n_d = sizes
    _, cx, cy, cz = forward_now.shape
    nrec = cells_given.shape[1]
    groups = cy // 8
    here = tuple(lax.axis_index(axis) for axis in AXES)
    rows = slice(TOP, TOP + cy)
    up = slice(TOP - 1, TOP + cy - 1)
    down = slice(TOP + 1, TOP + cy + 1)
    top = n_d - 1
    leader = here[2] == top
    nows = (forward_now, adjoint_now)

    def present(direction):
        ok = None
        for at, step, size in zip(here, direction, sizes):
            if step == 0:
                continue
            this = (at < size - 1) if step > 0 else (at > 0)
            ok = this if ok is None else jnp.logical_and(ok, this)
        return ok

    def target(direction, depth):
        place = {axis: at + step for axis, at, step in zip(AXES, here, direction) if step != 0}
        return {**place, "depth": depth}

    def opposite(d):
        return tuple(-step for step in d)

    live = [d for d in DIRECTIONS if all(s == 0 or n > 1 for s, n in zip(d, sizes))]
    peers = [(a, b) for a in range(n_in) for b in range(n_x) if (a, b) != (0, 0)]

    def peer(k):
        return {
            "inline": lax.rem(here[0] + peers[k][0], n_in),
            "xline": lax.rem(here[1] + peers[k][1], n_x),
        }

    def at_depth(depth):
        return {"depth": depth}

    inputs = [
        (forward_now, lambda t: fields.at[1, 0, :, pl.ds(1, cx), t, pl.ds(TOP, cy)]),
        (courant, lambda t: model.at[0, :, t]),
        (epsilon, lambda t: model.at[1, :, t]),
        (delta, lambda t: model.at[2, :, t]),
        (tilt_class, lambda t: classes.at[0, :, t]),
        (azimuth_class, lambda t: classes.at[1, :, t]),
        (forward_before, lambda t: fields.at[0, 0, :, pl.ds(1, cx), t, pl.ds(TOP, cy)]),
        (adjoint_now, lambda t: fields.at[1, 1, :, pl.ds(1, cx), t, pl.ds(TOP, cy)]),
        (adjoint_before, lambda t: fields.at[0, 1, :, pl.ds(1, cx), t, pl.ds(TOP, cy)]),
    ]

    def load(number):
        source, place = inputs[number]
        return pltpu.make_async_copy(source, place(top), load_sem.at[number])

    smalls = [
        (cells_given, receiver_cells),
        (data_given, receiver_data),
        (tilt_given, tilt_table),
        (azimuth_given, azimuth_table),
        (source_given, source_cell),
        (wavelet_given, wavelet),
    ]

    def small(number):
        source, place = smalls[number]
        return pltpu.make_async_copy(source, place, small_sem.at[number])

    def ship(number, t):
        source, place = inputs[number]
        return pltpu.make_async_remote_copy(
            src_ref=source,
            dst_ref=place(t),
            send_sem=ship_send.at[number],
            recv_sem=ship_recv.at[t, number],
            device_id=at_depth(top),
            device_id_type=MESH,
        )

    def wait_input(number):
        load(number).wait()
        for t in range(top):
            ship(number, t).wait_recv()

    def edge(step, size, first):
        if step == 0:
            return pl.ds(first, size)
        return pl.ds(first + size - 1 if step > 0 else first, 1)

    def beyond(step, size, first):
        if step == 0:
            return pl.ds(first, size)
        return pl.ds(first - 1 if step > 0 else first + size, 1)

    def first_copy(d, system, t):
        return pltpu.make_async_remote_copy(
            src_ref=nows[system].at[:, edge(d[0], cx, 0), edge(d[1], cy, 0)],
            dst_ref=fields.at[1, system, :, beyond(d[0], cx, 1), t, beyond(d[1], cy, TOP)],
            send_sem=first_send.at[system, DIRECTIONS.index(d)],
            recv_sem=first_recv.at[t, system, DIRECTIONS.index(d)],
            device_id=target(d, top),
            device_id_type=MESH,
        )

    def halo_copy(d, s, system):
        return pltpu.make_async_remote_copy(
            src_ref=fields.at[s + 1, system, :, edge(d[0], cx, 1), :, edge(d[1], cy, TOP)],
            dst_ref=fields.at[s + 1, system, :, beyond(d[0], cx, 1), :, beyond(d[1], cy, TOP)],
            send_sem=halo_send.at[s, system, DIRECTIONS.index(d)],
            recv_sem=halo_recv.at[s, system, DIRECTIONS.index(d)],
            device_id=target(d, top),
            device_id_type=MESH,
        )

    def trace_copy(s, k):
        return pltpu.make_async_remote_copy(
            src_ref=trace_own.at[s],
            dst_ref=trace_got.at[s, k],
            send_sem=trace_send.at[s, k],
            recv_sem=trace_recv.at[s, k],
            device_id=peer(k),
            device_id_type=MESH,
        )

    results = [
        (lambda t: fields.at[STEPS + 1, 0, :, pl.ds(1, cx), t, pl.ds(TOP, cy)], forward_out),
        (lambda t: fields.at[STEPS + 1, 1, :, pl.ds(1, cx), t, pl.ds(TOP, cy)], adjoint_out),
        (lambda t: image.at[t], image_out),
        (lambda t: trace_all, traces_out),
    ]

    def result_copy(number, t):
        source, place = results[number]
        return pltpu.make_async_remote_copy(
            src_ref=source(t),
            dst_ref=place,
            send_sem=result_send.at[number, t],
            recv_sem=result_recv.at[number],
            device_id=at_depth(t),
            device_id_type=MESH,
        )

    def give_result(number):
        for t in range(top):
            result_copy(number, t).start()

    barrier = pltpu.get_barrier_semaphore()

    def greet(place):
        pl.semaphore_signal(barrier, inc=1, device_id=place, device_id_type=MESH)

    def send_first(t, system):
        for d in sorted(live, key=lambda d: (d[0] == 0, d[1] != 0)):

            @pl.when(present(d))
            def _(d=d):
                first_copy(d, system, t).start()

    def drain_first(t):
        for system in range(2):
            for d in live:

                @pl.when(present(d))
                def _(d=d):
                    first_copy(d, system, t).wait_send()

    def clear(d):
        for s in range(STEPS):
            for system in range(2):
                place = fields.at[
                    s + 1, system, :, beyond(d[0], cx, 1), :, beyond(d[1], cy, TOP)
                ]
                place[...] = jnp.zeros(place.shape, jnp.float32)

    def clear_absent():
        for d in DIRECTIONS:
            if d not in live:
                clear(d)
            else:

                @pl.when(jnp.logical_not(present(opposite(d))))
                def _(d=d):
                    clear(d)

    def send(s, system, which):
        for d in which:
            if d in live:

                @pl.when(present(d))
                def _(d=d):
                    halo_copy(d, s, system).start()

    def receive(s, system, which):
        for d in which:
            if d in live:

                @pl.when(present(opposite(d)))
                def _(d=d):
                    if s == 0:
                        for t in range(n_d):
                            first_copy(d, system, t).wait_recv()
                    else:
                        halo_copy(d, s, system).wait_recv()

    def drain(s, system):
        for d in live:

            @pl.when(present(d))
            def _(d=d):
                halo_copy(d, s, system).wait_send()

    lane = lax.broadcasted_iota(jnp.int32, (8, LANES), 1)
    first_lane, last_lane = lane == 0, lane == LANES - 1

    def along_depth(s, system, f, plane, row):
        tiles = [fields[s + 1, system, f, plane, t, row : row + 8, :] for t in range(n_d)]
        right = [pltpu.roll(tile, 1, 1) for tile in tiles]
        left = [pltpu.roll(tile, LANES - 1, 1) for tile in tiles]
        before = [
            jnp.where(first_lane, right[t - 1] if t > 0 else 0.0, right[t]) for t in range(n_d)
        ]
        after = [
            jnp.where(last_lane, left[t + 1] if t < top else 0.0, left[t]) for t in range(n_d)
        ]
        return before, after

    def own_depth(s, system):
        for f in range(2):
            for i in range(cx):
                for r in range(groups):
                    before, after = along_depth(s, system, f, i + 1, TOP + 8 * r)
                    for t in range(n_d):
                        at = slice(TOP + 8 * r, TOP + 8 * r + 8)
                        zdiff[system, f, i + 1, t, at, :] = after[t] - before[t]
                        zsum[system, f, i, t, 8 * r : 8 * r + 8, :] = after[t] + before[t]

    def side_depth(s, system):
        for f in range(2):
            for i in range(cx):
                for row in (0, TOP + cy):
                    before, after = along_depth(s, system, f, i + 1, row)
                    for t in range(n_d):
                        zdiff[system, f, i + 1, t, row : row + 8, :] = after[t] - before[t]

    def face_depth(s, system, plane):
        for f in range(2):
            for r in range(groups):
                before, after = along_depth(s, system, f, plane, TOP + 8 * r)
                for t in range(n_d):
                    at = slice(TOP + 8 * r, TOP + 8 * r + 8)
                    zdiff[system, f, plane, t, at, :] = after[t] - before[t]

    outer = sorted({0, cx - 1})
    inner = [i for i in range(cx) if i not in outer]

    def advance(s, system, i):
        for t in range(n_d):
            axial = []
            lap = None
            doubled = []
            for f in range(2):
                now = fields.at[s + 1, system, f]
                slope = zdiff.at[system, f]
                twice = 2.0 * now[i + 1, t, rows, :]
                doubled.append(twice)
                dxx = now[i + 2, t, rows, :] + now[i, t, rows, :] - twice
                dyy = now[i + 1, t, down, :] + now[i + 1, t, up, :] - twice
                dzz = zsum[system, f, i, t] - twice
                dxy = (
                    now[i + 2, t, down, :]
                    - now[i + 2, t, up, :]
                    - now[i, t, down, :]
                    + now[i, t, up, :]
                )
                dxz = slope[i + 2, t, rows, :] - slope[i, t, rows, :]
                dyz = slope[i + 1, t, down, :] - slope[i + 1, t, up, :]
                axial.append(
                    factors[3, i, t] * dxx
                    + factors[4, i, t] * dyy
                    + factors[5, i, t] * dzz
                    + factors[6, i, t] * dxy
                    + factors[7, i, t] * dxz
                    + factors[8, i, t] * dyz
                )
                if f == 0:
                    lap = dxx + dyy + dzz
            plane_part = lap - axial[0]
            along = factors[2, i, t] * axial[1]
            if system == 0:
                row_at = lax.broadcasted_iota(jnp.int32, (cy, LANES), 0)
                lane_at = lax.broadcasted_iota(jnp.int32, (cy, LANES), 1)
                cell = (
                    (here[0] * cx + i) * (n_x * cy) + here[1] * cy + row_at
                ) * (n_d * cz) + t * cz + lane_at
                added = jnp.where(cell == source_cell[0], wavelet[s], 0.0)
            else:
                added = terms[s, i, t]
            new = []
            for f in range(2):
                value = (
                    doubled[f]
                    - fields[s, system, f, i + 1, t, rows, :]
                    + factors[f, i, t] * plane_part
                    + along
                    + added
                )
                fields[s + 2, system, f, i + 1, t, rows, :] = value
                new.append(value)
            if system == 1:
                product = (
                    fields[s + 2, 0, 0, i + 1, t, rows, :] * new[0]
                    + fields[s + 2, 0, 1, i + 1, t, rows, :] * new[1]
                )
                if s > 0:
                    product = image[t, i] + product
                if s == STEPS - 1 and t == top:
                    image_out[i] = product
                else:
                    image[t, i] = product
            if s == STEPS - 1 and t == top:
                out = forward_out if system == 0 else adjoint_out
                out[0, i] = new[0]
                out[1, i] = new[1]

    def coefficients():
        tilt_sine, tilt_cosine = jnp.sin(tilt_table[...]), jnp.cos(tilt_table[...])
        turn_sine, turn_cosine = jnp.sin(azimuth_table[...]), jnp.cos(azimuth_table[...])

        def spread_out(values):
            wide_table = jnp.zeros((8, LANES), jnp.float32)
            for k in range(values.shape[1]):
                wide_table = jnp.where(
                    lane == k, jnp.broadcast_to(values[:, k : k + 1], (8, LANES)), wide_table
                )
            return wide_table

        tilt_tables = [spread_out(v) for v in (tilt_sine, tilt_cosine)]
        turn_tables = [spread_out(v) for v in (turn_cosine, turn_sine)]

        def look(which, i, t, tables):
            found = [[] for _ in tables]
            for r in range(groups):
                chosen = classes[which, i, t, 8 * r : 8 * r + 8, :]
                for table, parts in zip(tables, found):
                    parts.append(jnp.take_along_axis(table, chosen, axis=1))
            return [jnp.concatenate(parts, axis=0) for parts in found]

        for i in range(cx):
            for t in range(n_d):
                sine, third = look(0, i, t, tilt_tables)
                turned, across = look(1, i, t, turn_tables)
                first, second = sine * turned, sine * across
                base = model[0, i, t]
                factors[0, i, t] = base * (1.0 + 2.0 * model[1, i, t])
                factors[1, i, t] = base * (1.0 + 2.0 * model[2, i, t])
                factors[2, i, t] = base
                factors[3, i, t] = first * first
                factors[4, i, t] = second * second
                factors[5, i, t] = third * third
                factors[6, i, t] = 0.5 * first * second
                factors[7, i, t] = 0.5 * first * third
                factors[8, i, t] = 0.5 * second * third

    volume = cx * cy
    wide = n_d * cz

    def receivers():
        cells = receiver_cells[...]
        upper, depth_at = split_by(cells, wide)
        inline_at, xline_at = split_by(upper, n_x * cy)
        inline_at = inline_at - here[0] * cx
        xline_at = xline_at - here[1] * cy
        inside = (inline_at >= 0) & (inline_at < cx) & (xline_at >= 0) & (xline_at < cy)
        row_of = jnp.where(inside, inline_at * cy + xline_at, -1)
        row_match = (
            lax.broadcasted_iota(jnp.int32, (volume, nrec), 0)
            == jnp.broadcast_to(row_of, (volume, nrec))
        )
        lane_match = (
            lax.broadcasted_iota(jnp.int32, (wide, nrec), 0)
            == jnp.broadcast_to(depth_at, (wide, nrec))
        )
        hot_row[...] = jnp.where(row_match, 1.0, 0.0)
        lanes_hot = jnp.where(lane_match, 1.0, 0.0).astype(jnp.bfloat16)
        for part in range(2):
            hot_lane[part * wide : (part + 1) * wide, :] = lanes_hot

    def injection(s):
        for number, part in enumerate(two_parts(receiver_data[s : s + 1, :])):
            spread[number * volume : (number + 1) * volume, :] = hot_row[...].astype(
                jnp.bfloat16
            ) * jnp.broadcast_to(part, (volume, nrec))
        got = lax.dot_general(
            spread[...],
            hot_lane[0:wide, :],
            (((1,), (1,)), ((), ())),
            preferred_element_type=jnp.float32,
        )
        total = got[:volume] + got[volume:]
        for i in range(cx):
            for t in range(n_d):
                terms[s, i, t] = total[i * cy : (i + 1) * cy, t * cz : (t + 1) * cz]

    def sample(s):
        tiles = [
            jnp.concatenate(
                [fields[s + 2, 0, 0, i + 1, t, rows, :] for i in range(cx)], axis=0
            )
            for t in range(n_d)
        ]
        split = [two_parts(tile) for tile in tiles]
        parts = jnp.concatenate(
            [split[t][part] for part in range(2) for t in range(n_d)], axis=1
        )
        picked = jnp.dot(parts, hot_lane[...], preferred_element_type=jnp.float32)
        trace_own[s] = jnp.sum(picked * hot_row[...], axis=0, keepdims=True)

    def share(s):
        for k in range(len(peers)):
            trace_copy(s, k).start()

    def finish_trace(s):
        total = trace_own[s]
        for k in range(len(peers)):
            trace_copy(s, k).wait_recv()
            total = total + trace_got[s, k]
            if s < STEPS - 1:
                trace_copy(s, k).wait_send()
        traces_out[s : s + 1, :] = total
        trace_all[s : s + 1, :] = total

    @pl.when(jnp.logical_not(leader))
    def _():
        greet(at_depth(top))
        expected = jnp.int32(1)
        for d in live:
            expected = expected + jnp.where(present(d), 1, 0)
        pl.semaphore_wait(barrier, expected)
        send_first(here[2], 0)
        for number in range(len(inputs)):
            if number == 7:
                send_first(here[2], 1)
            ship(number, here[2]).start()
        for number in range(len(inputs)):
            ship(number, here[2]).wait_send()
        drain_first(here[2])
        for number in range(len(results)):
            result_copy(number, here[2]).wait_recv()

    @pl.when(leader)
    def _():
        for d in live:

            @pl.when(present(d))
            def _(d=d):
                for t in range(top):
                    greet(target(d, t))

        for k in range(len(peers)):
            greet(peer(k))
        for t in range(top):
            greet(at_depth(t))
        for number in range(len(smalls)):
            small(number).start()
        for number in range(len(inputs)):
            load(number).start()
        pl.semaphore_wait(barrier, len(peers) + top)
        for system in range(2):
            send_first(top, system)
        clear_absent()
        for number in range(len(smalls)):
            small(number).wait()
        receivers()
        for number in range(1, 6):
            wait_input(number)
        coefficients()
        wait_input(0)
        own_depth(0, 0)
        wait_input(6)
        for s in range(STEPS):
            for system in range(2):
                if s == 0 and system == 1:
                    wait_input(7)
                    own_depth(0, 1)
                    wait_input(8)
                    injection(0)
                receive(s, system, SIDES)
                side_depth(s, system)
                for i in inner:
                    advance(s, system, i)
                if cx > 1:
                    for i, side in ((0, 1), (cx - 1, -1)):
                        receive(s, system, [d for d in FACES if d[0] == side])
                        face_depth(s, system, 0 if side > 0 else cx + 1)
                        advance(s, system, i)
                        if s < STEPS - 1:
                            send(s + 1, system, [d for d in FACES if d[0] == -side])
                else:
                    receive(s, system, FACES)
                    for plane in (0, cx + 1):
                        face_depth(s, system, plane)
                    advance(s, system, 0)
                    if s < STEPS - 1:
                        send(s + 1, system, FACES)
                if s < STEPS - 1:
                    send(s + 1, system, SIDES)
                else:
                    if system == 0:
                        sample(s)
                        share(s)
                    give_result(system)
            if s < STEPS - 1:
                own_depth(s + 1, 0)
                own_depth(s + 1, 1)
                sample(s)
                share(s)
                injection(s + 1)
                if s == 0:
                    drain_first(top)
                else:
                    for system in range(2):
                        drain(s, system)
                    finish_trace(s - 1)
        give_result(2)
        for system in range(2):
            drain(STEPS - 1, system)
        for s in range(STEPS - 2, STEPS):
            finish_trace(s)
        give_result(3)
        for k in range(len(peers)):
            trace_copy(STEPS - 1, k).wait_send()
        for number in range(len(results)):
            for t in range(top):
                result_copy(number, t).wait_send()


def publish(*refs):
    half = len(refs) // 2
    for source, place in zip(refs[:half], refs[half:]):
        place[...] = source[...]


def per_device(sizes, *operands):
    shapes = [operand.shape for operand in operands]
    _, cx, cy, cz = shapes[0]
    nrec = shapes[13][0]
    n_in, n_x, n_d = sizes
    operands = list(operands)
    for which in (9, 10, 13):
        operands[which] = operands[which].reshape(1, -1)
    f32, bf16 = jnp.float32, jnp.bfloat16
    padded = cy + 2 * TOP
    chips = n_in * n_x
    count = len(DIRECTIONS)
    dma = pltpu.SemaphoreType.DMA
    scratch = [
        pltpu.VMEM((STEPS + 2, 2, 2, cx + 2, n_d, padded, cz), f32),
        pltpu.VMEM((3, cx, n_d, cy, cz), f32),
        pltpu.VMEM((2, cx, n_d, cy, cz), jnp.int32),
        pltpu.VMEM((9, cx, n_d, cy, cz), f32),
        pltpu.VMEM((2, 2, cx + 2, n_d, padded, cz), f32),
        pltpu.VMEM((2, 2, cx, n_d, cy, cz), f32),
        pltpu.VMEM((n_d, cx, cy, cz), f32),
        pltpu.VMEM(operands[9].shape, f32),
        pltpu.VMEM(operands[10].shape, f32),
        pltpu.SMEM(shapes[11], jnp.int32),
        pltpu.SMEM(shapes[12], f32),
        pltpu.VMEM(operands[13].shape, jnp.int32),
        pltpu.VMEM(shapes[14], f32),
        pltpu.VMEM((cx * cy, nrec), f32),
        pltpu.VMEM((2 * n_d * cz, nrec), bf16),
        pltpu.VMEM((2 * cx * cy, nrec), bf16),
        pltpu.VMEM((STEPS, cx, n_d, cy, cz), f32),
        pltpu.VMEM((STEPS, 1, nrec), f32),
        pltpu.VMEM((STEPS, chips, 1, nrec), f32),
        pltpu.VMEM((STEPS, nrec), f32),
        dma((9,)),
        dma((6,)),
        dma((9,)),
        dma((n_d, 9)),
        dma((2, count)),
        dma((n_d, 2, count)),
        dma((STEPS, 2, count)),
        dma((STEPS, 2, count)),
        dma((STEPS, chips)),
        dma((STEPS, chips)),
        dma((4, n_d)),
        dma((4,)),
    ]
    vmem = pl.BlockSpec(memory_space=pltpu.VMEM)
    anywhere = pl.BlockSpec(memory_space=pl.ANY)
    made = pl.pallas_call(
        functools.partial(kernel, sizes),
        out_shape=(
            pltpu.VMEM((2, cx, cy, cz), f32),
            pltpu.VMEM((2, cx, cy, cz), f32),
            pltpu.VMEM((cx, cy, cz), f32),
            pltpu.VMEM((STEPS, nrec), f32),
        ),
        in_specs=[anywhere] * len(operands),
        out_specs=(vmem, vmem, vmem, vmem),
        scratch_shapes=scratch,
        compiler_params=pltpu.CompilerParams(
            collective_id=0, has_side_effects=True, vmem_limit_bytes=56 * 2**20
        ),
        name="wavefields",
    )(*operands)
    return pl.pallas_call(
        publish,
        out_shape=[jax.ShapeDtypeStruct(m.shape, m.dtype) for m in made],
        in_specs=[vmem] * len(made),
        out_specs=[vmem] * len(made),
        compiler_params=pltpu.CompilerParams(vmem_limit_bytes=4 * 2**20),
        name="publish",
    )(*made)


def solution(mesh):
    sizes = tuple(mesh.shape[axis] for axis in AXES)
    field = P(None, ("shot", "inline"), "xline", "depth")
    cell = P("inline", "xline", "depth")
    return jax.shard_map(
        functools.partial(per_device, sizes),
        mesh=mesh,
        in_specs=(
            field, field, field, field,
            cell, cell, cell, cell, cell,
            P(), P(), P("shot"), P("shot"), P("shot"), P(None, "shot"),
        ),
        out_specs=(field, field, P(("shot", "inline"), "xline", "depth"), P(None, "shot")),
        check_vma=False,
    )
```

```python
import functools

import jax
import jax.numpy as jnp
from jax import lax
from jax.experimental import pallas as pl
from jax.experimental.pallas import tpu as pltpu
from jax.sharding import PartitionSpec as P

STEPS = 4
MESH = pl.DeviceIdType.MESH
AXES = ("inline", "xline", "depth")
LANES = 128
TOP = 8

DIRECTIONS = [(a, b) for a in (-1, 0, 1) for b in (-1, 0, 1) if (a, b) != (0, 0)]
SIDES = [d for d in DIRECTIONS if d[0] == 0]
FACES = [d for d in DIRECTIONS if d[0] != 0]


def split_by(values, size):
    if size & (size - 1) == 0:
        return values >> (size.bit_length() - 1), values & (size - 1)
    quotient = lax.div(values, jnp.int32(size))
    return quotient, values - quotient * size


def two_parts(values):
    high = values.astype(jnp.bfloat16)
    return high, (values - high.astype(jnp.float32)).astype(jnp.bfloat16)


def kernel(
    sizes,
    forward_now,
    forward_before,
    adjoint_now,
    adjoint_before,
    courant,
    epsilon,
    delta,
    tilt_class,
    azimuth_class,
    tilt_given,
    azimuth_given,
    source_given,
    wavelet_given,
    cells_given,
    data_given,
    forward_out,
    adjoint_out,
    image_out,
    traces_out,
    fields,
    model,
    classes,
    factors,
    zdiff,
    zsum,
    image,
    tilt_table,
    azimuth_table,
    source_cell,
    wavelet,
    receiver_cells,
    receiver_data,
    hot_row,
    hot_lane,
    spread,
    terms,
    trace_own,
    trace_got,
    trace_all,
    load_sem,
    small_sem,
    ship_send,
    ship_recv,
    first_send,
    first_recv,
    halo_send,
    halo_recv,
    trace_send,
    trace_recv,
    terms_send,
    terms_recv,
    result_send,
    result_recv,
):
    n_in, n_x, n_d = sizes
    _, cx, cy, cz = forward_now.shape
    nrec = cells_given.shape[1]
    groups = cy // 8
    here = tuple(lax.axis_index(axis) for axis in AXES)
    rows = slice(TOP, TOP + cy)
    up = slice(TOP - 1, TOP + cy - 1)
    down = slice(TOP + 1, TOP + cy + 1)
    top = n_d - 1
    leader = here[2] == top

    def present(direction):
        ok = None
        for at, step, size in zip(here, direction, sizes):
            if step == 0:
                continue
            this = (at < size - 1) if step > 0 else (at > 0)
            ok = this if ok is None else jnp.logical_and(ok, this)
        return ok

    def target(direction, depth):
        place = {axis: at + step for axis, at, step in zip(AXES, here, direction) if step != 0}
        return {**place, "depth": depth}

    def opposite(d):
        return tuple(-step for step in d)

    live = [d for d in DIRECTIONS if all(s == 0 or n > 1 for s, n in zip(d, sizes))]
    peers = [(a, b) for a in range(n_in) for b in range(n_x) if (a, b) != (0, 0)]

    def peer(k):
        return {
            "inline": lax.rem(here[0] + peers[k][0], n_in),
            "xline": lax.rem(here[1] + peers[k][1], n_x),
        }

    def at_depth(depth):
        return {"depth": depth}

    inputs = [
        (forward_now, lambda t: fields.at[1, 0, :, pl.ds(1, cx), t, pl.ds(TOP, cy)]),
        (courant, lambda t: model.at[0, :, t]),
        (epsilon, lambda t: model.at[1, :, t]),
        (delta, lambda t: model.at[2, :, t]),
        (tilt_class, lambda t: classes.at[0, :, t]),
        (azimuth_class, lambda t: classes.at[1, :, t]),
        (forward_before, lambda t: fields.at[0, 0, :, pl.ds(1, cx), t, pl.ds(TOP, cy)]),
        (adjoint_now, lambda t: fields.at[1, 1, :, pl.ds(1, cx), t, pl.ds(TOP, cy)]),
        (adjoint_before, lambda t: fields.at[0, 1, :, pl.ds(1, cx), t, pl.ds(TOP, cy)]),
    ]

    nows = (0, 7)

    def load(number, t):
        source, place = inputs[number]
        return pltpu.make_async_copy(source, place(t), load_sem.at[number])

    smalls = [
        (cells_given, receiver_cells),
        (data_given, receiver_data),
        (tilt_given, tilt_table),
        (azimuth_given, azimuth_table),
        (source_given, source_cell),
        (wavelet_given, wavelet),
    ]

    def small(number):
        source, place = smalls[number]
        return pltpu.make_async_copy(source, place, small_sem.at[number])

    def ship(number, t):
        source, place = inputs[number]
        return pltpu.make_async_remote_copy(
            src_ref=source,
            dst_ref=place(t),
            send_sem=ship_send.at[number],
            recv_sem=ship_recv.at[t, number],
            device_id=at_depth(top),
            device_id_type=MESH,
        )

    def wait_input(number):
        if number not in nows:
            load(number, top).wait()
        for t in range(top):
            ship(number, t).wait_recv()

    def edge(step, size, first):
        if step == 0:
            return pl.ds(first, size)
        return pl.ds(first + size - 1 if step > 0 else first, 1)

    def beyond(step, size, first):
        if step == 0:
            return pl.ds(first, size)
        return pl.ds(first - 1 if step > 0 else first + size, 1)

    def first_copy(d, system, t):
        return pltpu.make_async_remote_copy(
            src_ref=fields.at[1, system, :, edge(d[0], cx, 1), t, edge(d[1], cy, TOP)],
            dst_ref=fields.at[1, system, :, beyond(d[0], cx, 1), t, beyond(d[1], cy, TOP)],
            send_sem=first_send.at[system, DIRECTIONS.index(d)],
            recv_sem=first_recv.at[t, system, DIRECTIONS.index(d)],
            device_id=target(d, top),
            device_id_type=MESH,
        )

    def halo_copy(d, s, system):
        return pltpu.make_async_remote_copy(
            src_ref=fields.at[s + 1, system, :, edge(d[0], cx, 1), :, edge(d[1], cy, TOP)],
            dst_ref=fields.at[s + 1, system, :, beyond(d[0], cx, 1), :, beyond(d[1], cy, TOP)],
            send_sem=halo_send.at[s, system, DIRECTIONS.index(d)],
            recv_sem=halo_recv.at[s, system, DIRECTIONS.index(d)],
            device_id=target(d, top),
            device_id_type=MESH,
        )

    def trace_copy(late, k):
        steps = pl.ds(STEPS - 1, 1) if late else pl.ds(0, STEPS - 1)
        return pltpu.make_async_remote_copy(
            src_ref=trace_own.at[steps],
            dst_ref=trace_got.at[k, steps],
            send_sem=trace_send.at[late, k],
            recv_sem=trace_recv.at[late, k],
            device_id=peer(k),
            device_id_type=MESH,
        )

    results = [
        (lambda t: fields.at[STEPS + 1, 0, :, pl.ds(1, cx), t, pl.ds(TOP, cy)], forward_out),
        (lambda t: fields.at[STEPS + 1, 1, :, pl.ds(1, cx), t, pl.ds(TOP, cy)], adjoint_out),
        (lambda t: image.at[t], image_out),
        (lambda t: trace_all, traces_out),
    ]

    def result_copy(number, t):
        source, place = results[number]
        return pltpu.make_async_remote_copy(
            src_ref=source(t),
            dst_ref=place,
            send_sem=result_send.at[number, t],
            recv_sem=result_recv.at[number],
            device_id=at_depth(t),
            device_id_type=MESH,
        )

    def give_result(number):
        for t in range(top):
            result_copy(number, t).start()

    barrier = pltpu.get_barrier_semaphore()

    def greet(place):
        pl.semaphore_signal(barrier, inc=1, device_id=place, device_id_type=MESH)

    def send_first(t, system):
        for d in sorted(live, key=lambda d: (d[0] == 0, d[1] != 0)):

            @pl.when(present(d))
            def _(d=d):
                first_copy(d, system, t).start()

    def drain_first(t):
        for system in range(2):
            for d in live:

                @pl.when(present(d))
                def _(d=d):
                    first_copy(d, system, t).wait_send()

    def clear(d):
        for s in range(STEPS):
            for system in range(2):
                place = fields.at[
                    s + 1, system, :, beyond(d[0], cx, 1), :, beyond(d[1], cy, TOP)
                ]
                place[...] = jnp.zeros(place.shape, jnp.float32)

    def clear_absent():
        for d in DIRECTIONS:
            if d not in live:
                clear(d)
            else:

                @pl.when(jnp.logical_not(present(opposite(d))))
                def _(d=d):
                    clear(d)

    def send(s, system, which):
        for d in which:
            if d in live:

                @pl.when(present(d))
                def _(d=d):
                    halo_copy(d, s, system).start()

    def receive(s, system, which):
        for d in which:
            if d in live:

                @pl.when(present(opposite(d)))
                def _(d=d):
                    if s == 0:
                        for t in range(n_d):
                            first_copy(d, system, t).wait_recv()
                    else:
                        halo_copy(d, s, system).wait_recv()

    def drain(s, system):
        for d in live:

            @pl.when(present(d))
            def _(d=d):
                halo_copy(d, s, system).wait_send()

    lane = lax.broadcasted_iota(jnp.int32, (8, LANES), 1)
    first_lane, last_lane = lane == 0, lane == LANES - 1

    def along_depth(s, system, f, plane, row):
        tiles = [fields[s + 1, system, f, plane, t, row : row + 8, :] for t in range(n_d)]
        right = [pltpu.roll(tile, 1, 1) for tile in tiles]
        left = [pltpu.roll(tile, LANES - 1, 1) for tile in tiles]
        before = [
            jnp.where(first_lane, right[t - 1] if t > 0 else 0.0, right[t]) for t in range(n_d)
        ]
        after = [
            jnp.where(last_lane, left[t + 1] if t < top else 0.0, left[t]) for t in range(n_d)
        ]
        return before, after

    def own_depth(s, system):
        for f in range(2):
            for i in range(cx):
                for r in range(groups):
                    before, after = along_depth(s, system, f, i + 1, TOP + 8 * r)
                    for t in range(n_d):
                        at = slice(TOP + 8 * r, TOP + 8 * r + 8)
                        zdiff[system, f, i + 1, t, at, :] = after[t] - before[t]
                        zsum[system, f, i, t, 8 * r : 8 * r + 8, :] = after[t] + before[t]

    def side_depth(s, system):
        for f in range(2):
            for i in range(cx):
                for row in (0, TOP + cy):
                    before, after = along_depth(s, system, f, i + 1, row)
                    for t in range(n_d):
                        zdiff[system, f, i + 1, t, row : row + 8, :] = after[t] - before[t]

    def face_depth(s, system, plane):
        for f in range(2):
            for r in range(groups):
                before, after = along_depth(s, system, f, plane, TOP + 8 * r)
                for t in range(n_d):
                    at = slice(TOP + 8 * r, TOP + 8 * r + 8)
                    zdiff[system, f, plane, t, at, :] = after[t] - before[t]

    outer = sorted({0, cx - 1})
    inner = [i for i in range(cx) if i not in outer]

    def advance(s, system, i):
        for t in range(n_d):
            axial = []
            lap = None
            doubled = []
            for f in range(2):
                now = fields.at[s + 1, system, f]
                slope = zdiff.at[system, f]
                twice = 2.0 * now[i + 1, t, rows, :]
                doubled.append(twice)
                dxx = now[i + 2, t, rows, :] + now[i, t, rows, :] - twice
                dyy = now[i + 1, t, down, :] + now[i + 1, t, up, :] - twice
                dzz = zsum[system, f, i, t] - twice
                dxy = (
                    now[i + 2, t, down, :]
                    - now[i + 2, t, up, :]
                    - now[i, t, down, :]
                    + now[i, t, up, :]
                )
                dxz = slope[i + 2, t, rows, :] - slope[i, t, rows, :]
                dyz = slope[i + 1, t, down, :] - slope[i + 1, t, up, :]
                axial.append(
                    factors[3, i, t] * dxx
                    + factors[4, i, t] * dyy
                    + factors[5, i, t] * dzz
                    + factors[6, i, t] * dxy
                    + factors[7, i, t] * dxz
                    + factors[8, i, t] * dyz
                )
                if f == 0:
                    lap = dxx + dyy + dzz
            plane_part = lap - axial[0]
            along = factors[2, i, t] * axial[1]
            if system == 0:
                row_at = lax.broadcasted_iota(jnp.int32, (cy, LANES), 0)
                lane_at = lax.broadcasted_iota(jnp.int32, (cy, LANES), 1)
                cell = (
                    (here[0] * cx + i) * (n_x * cy) + here[1] * cy + row_at
                ) * (n_d * cz) + t * cz + lane_at
                added = jnp.where(cell == source_cell[0], wavelet[s], 0.0)
            else:
                added = terms[s, i, t]
            new = []
            for f in range(2):
                value = (
                    doubled[f]
                    - fields[s, system, f, i + 1, t, rows, :]
                    + factors[f, i, t] * plane_part
                    + along
                    + added
                )
                fields[s + 2, system, f, i + 1, t, rows, :] = value
                new.append(value)
            if system == 1:
                product = (
                    fields[s + 2, 0, 0, i + 1, t, rows, :] * new[0]
                    + fields[s + 2, 0, 1, i + 1, t, rows, :] * new[1]
                )
                if s > 0:
                    product = image[t, i] + product
                if s == STEPS - 1 and t == top:
                    image_out[i] = product
                else:
                    image[t, i] = product
            if s == STEPS - 1 and t == top:
                out = forward_out if system == 0 else adjoint_out
                out[0, i] = new[0]
                out[1, i] = new[1]

    def coefficients():
        tilt_sine, tilt_cosine = jnp.sin(tilt_table[...]), jnp.cos(tilt_table[...])
        turn_sine, turn_cosine = jnp.sin(azimuth_table[...]), jnp.cos(azimuth_table[...])

        def spread_out(values):
            wide_table = jnp.zeros((8, LANES), jnp.float32)
            for k in range(values.shape[1]):
                wide_table = jnp.where(
                    lane == k, jnp.broadcast_to(values[:, k : k + 1], (8, LANES)), wide_table
                )
            return wide_table

        tilt_tables = [spread_out(v) for v in (tilt_sine, tilt_cosine)]
        turn_tables = [spread_out(v) for v in (turn_cosine, turn_sine)]

        def look(which, i, t, tables):
            found = [[] for _ in tables]
            for r in range(groups):
                chosen = classes[which, i, t, 8 * r : 8 * r + 8, :]
                for table, parts in zip(tables, found):
                    parts.append(jnp.take_along_axis(table, chosen, axis=1))
            return [jnp.concatenate(parts, axis=0) for parts in found]

        for i in range(cx):
            for t in range(n_d):
                sine, third = look(0, i, t, tilt_tables)
                turned, across = look(1, i, t, turn_tables)
                first, second = sine * turned, sine * across
                base = model[0, i, t]
                factors[0, i, t] = base * (1.0 + 2.0 * model[1, i, t])
                factors[1, i, t] = base * (1.0 + 2.0 * model[2, i, t])
                factors[2, i, t] = base
                factors[3, i, t] = first * first
                factors[4, i, t] = second * second
                factors[5, i, t] = third * third
                factors[6, i, t] = 0.5 * first * second
                factors[7, i, t] = 0.5 * first * third
                factors[8, i, t] = 0.5 * second * third

    volume = cx * cy
    wide = n_d * cz

    def receivers():
        cells = receiver_cells[...]
        upper, depth_at = split_by(cells, wide)
        inline_at, xline_at = split_by(upper, n_x * cy)
        inline_at = inline_at - here[0] * cx
        xline_at = xline_at - here[1] * cy
        inside = (inline_at >= 0) & (inline_at < cx) & (xline_at >= 0) & (xline_at < cy)
        row_of = jnp.where(inside, inline_at * cy + xline_at, -1)
        row_match = (
            lax.broadcasted_iota(jnp.int32, (volume, nrec), 0)
            == jnp.broadcast_to(row_of, (volume, nrec))
        )
        lane_match = (
            lax.broadcasted_iota(jnp.int32, (wide, nrec), 0)
            == jnp.broadcast_to(depth_at, (wide, nrec))
        )
        hot_row[...] = jnp.where(row_match, 1.0, 0.0)
        lanes_hot = jnp.where(lane_match, 1.0, 0.0).astype(jnp.bfloat16)
        for part in range(2):
            hot_lane[part * wide : (part + 1) * wide, :] = lanes_hot

    def injection(s):
        for number, part in enumerate(two_parts(receiver_data[s : s + 1, :])):
            spread[number * volume : (number + 1) * volume, :] = hot_row[...].astype(
                jnp.bfloat16
            ) * jnp.broadcast_to(part, (volume, nrec))
        got = lax.dot_general(
            spread[...],
            hot_lane[0:wide, :],
            (((1,), (1,)), ((), ())),
            preferred_element_type=jnp.float32,
        )
        total = got[:volume] + got[volume:]
        for i in range(cx):
            for t in range(n_d):
                terms[s, i, t] = total[i * cy : (i + 1) * cy, t * cz : (t + 1) * cz]

    def sample(s):
        tiles = [
            jnp.concatenate(
                [fields[s + 2, 0, 0, i + 1, t, rows, :] for i in range(cx)], axis=0
            )
            for t in range(n_d)
        ]
        split = [two_parts(tile) for tile in tiles]
        parts = jnp.concatenate(
            [split[t][part] for part in range(2) for t in range(n_d)], axis=1
        )
        picked = jnp.dot(parts, hot_lane[...], preferred_element_type=jnp.float32)
        trace_own[s] = jnp.sum(picked * hot_row[...], axis=0, keepdims=True)

    def share(late):
        for k in range(len(peers)):
            trace_copy(late, k).start()

    def finish_trace(late):
        for k in range(len(peers)):
            trace_copy(late, k).wait_recv()
        for s in [STEPS - 1] if late else range(STEPS - 1):
            total = trace_own[s]
            for k in range(len(peers)):
                total = total + trace_got[k, s]
            traces_out[s : s + 1, :] = total
            trace_all[s : s + 1, :] = total

    def terms_copy(s):
        return pltpu.make_async_remote_copy(
            src_ref=terms.at[s],
            dst_ref=terms.at[s],
            send_sem=terms_send.at[s],
            recv_sem=terms_recv.at[s],
            device_id=at_depth(top),
            device_id_type=MESH,
        )

    nearby = max(n_in, n_x) <= STEPS
    neighbours = jnp.int32(0)
    for d in live:
        neighbours = neighbours + jnp.where(present(d), 1, 0)

    @pl.when(jnp.logical_not(leader))
    def _():
        greet(at_depth(top))
        for number in nows:
            load(number, here[2]).start()
        for number in (0, 1):
            small(number).start()
        for number in nows:
            load(number, here[2]).wait()
        pl.semaphore_wait(barrier, neighbours + 1)
        send_first(here[2], 0)
        for number in range(len(inputs)):
            if number == 7:
                send_first(here[2], 1)
            ship(number, here[2]).start()
        for number in (0, 1):
            small(number).wait()

        @pl.when(here[2] == 0)
        def _():
            receivers()
            for s in range(STEPS):
                injection(s)
                terms_copy(s).start()
            for s in range(STEPS):
                terms_copy(s).wait_send()

        for number in range(len(inputs)):
            ship(number, here[2]).wait_send()
        drain_first(here[2])
        for number in range(len(results)):
            result_copy(number, here[2]).wait_recv()

    @pl.when(leader)
    def _():
        for d in sorted(live, key=lambda d: d[0] * d[1] != 0):

            @pl.when(present(d))
            def _(d=d):
                for t in range(n_d if nearby else top):
                    greet(target(d, t))

        if not nearby:
            for k in range(len(peers)):
                greet(peer(k))
        for t in range(top):
            greet(at_depth(t))
        for number in nows:
            load(number, top).start()
        for number in range(len(smalls)):
            small(number).start()
        for number in range(len(inputs)):
            if number not in nows:
                load(number, top).start()
        for number in nows:
            load(number, top).wait()
        pl.semaphore_wait(barrier, (neighbours if nearby else len(peers)) + top)
        for system in range(2):
            send_first(top, system)
        clear_absent()
        for number in range(len(smalls)):
            small(number).wait()
        for number in range(1, 6):
            wait_input(number)
        coefficients()
        wait_input(0)
        own_depth(0, 0)
        receivers()
        wait_input(6)
        if top == 0:
            for s in range(STEPS):
                injection(s)
        for s in range(STEPS):
            for system in range(2):
                if s == 0 and system == 1:
                    wait_input(7)
                    own_depth(0, 1)
                    wait_input(8)
                if system == 1 and top > 0:
                    terms_copy(s).wait_recv()
                receive(s, system, SIDES)
                side_depth(s, system)
                for i in inner:
                    advance(s, system, i)
                if cx > 1:
                    for i, side in ((0, 1), (cx - 1, -1)):
                        receive(s, system, [d for d in FACES if d[0] == side])
                        face_depth(s, system, 0 if side > 0 else cx + 1)
                        advance(s, system, i)
                        if s < STEPS - 1:
                            send(s + 1, system, [d for d in FACES if d[0] == -side])
                else:
                    receive(s, system, FACES)
                    for plane in (0, cx + 1):
                        face_depth(s, system, plane)
                    advance(s, system, 0)
                    if s < STEPS - 1:
                        send(s + 1, system, FACES)
                if s < STEPS - 1:
                    send(s + 1, system, SIDES)
                    own_depth(s + 1, system)
                if system == 0:
                    sample(s)
                    if s == STEPS - 1:
                        share(1)
                elif s == STEPS - 2:
                    share(0)
                if s == STEPS - 1:
                    give_result(system)
            if s == 0:
                drain_first(top)
            else:
                for system in range(2):
                    drain(s, system)
        give_result(2)
        for late in range(2):
            finish_trace(late)
        give_result(3)
        for late in range(2):
            for k in range(len(peers)):
                trace_copy(late, k).wait_send()
        for number in range(len(results)):
            for t in range(top):
                result_copy(number, t).wait_send()


def publish(*refs):
    half = len(refs) // 2
    for source, place in zip(refs[:half], refs[half:]):
        place[...] = source[...]


def per_device(sizes, *operands):
    shapes = [operand.shape for operand in operands]
    _, cx, cy, cz = shapes[0]
    nrec = shapes[13][0]
    n_in, n_x, n_d = sizes
    operands = list(operands)
    for which in (9, 10, 13):
        operands[which] = operands[which].reshape(1, -1)
    f32, bf16 = jnp.float32, jnp.bfloat16
    padded = cy + 2 * TOP
    chips = n_in * n_x
    count = len(DIRECTIONS)
    dma = pltpu.SemaphoreType.DMA
    scratch = [
        pltpu.VMEM((STEPS + 2, 2, 2, cx + 2, n_d, padded, cz), f32),
        pltpu.VMEM((3, cx, n_d, cy, cz), f32),
        pltpu.VMEM((2, cx, n_d, cy, cz), jnp.int32),
        pltpu.VMEM((9, cx, n_d, cy, cz), f32),
        pltpu.VMEM((2, 2, cx + 2, n_d, padded, cz), f32),
        pltpu.VMEM((2, 2, cx, n_d, cy, cz), f32),
        pltpu.VMEM((n_d, cx, cy, cz), f32),
        pltpu.VMEM(operands[9].shape, f32),
        pltpu.VMEM(operands[10].shape, f32),
        pltpu.SMEM(shapes[11], jnp.int32),
        pltpu.SMEM(shapes[12], f32),
        pltpu.VMEM(operands[13].shape, jnp.int32),
        pltpu.VMEM(shapes[14], f32),
        pltpu.VMEM((cx * cy, nrec), f32),
        pltpu.VMEM((2 * n_d * cz, nrec), bf16),
        pltpu.VMEM((2 * cx * cy, nrec), bf16),
        pltpu.VMEM((STEPS, cx, n_d, cy, cz), f32),
        pltpu.VMEM((STEPS, 1, nrec), f32),
        pltpu.VMEM((chips, STEPS, 1, nrec), f32),
        pltpu.VMEM((STEPS, nrec), f32),
        dma((9,)),
        dma((6,)),
        dma((9,)),
        dma((n_d, 9)),
        dma((2, count)),
        dma((n_d, 2, count)),
        dma((STEPS, 2, count)),
        dma((STEPS, 2, count)),
        dma((2, chips)),
        dma((2, chips)),
        dma((STEPS,)),
        dma((STEPS,)),
        dma((4, n_d)),
        dma((4,)),
    ]
    vmem = pl.BlockSpec(memory_space=pltpu.VMEM)
    anywhere = pl.BlockSpec(memory_space=pl.ANY)
    made = pl.pallas_call(
        functools.partial(kernel, sizes),
        out_shape=(
            pltpu.VMEM((2, cx, cy, cz), f32),
            pltpu.VMEM((2, cx, cy, cz), f32),
            pltpu.VMEM((cx, cy, cz), f32),
            pltpu.VMEM((STEPS, nrec), f32),
        ),
        in_specs=[anywhere] * len(operands),
        out_specs=(vmem, vmem, vmem, vmem),
        scratch_shapes=scratch,
        compiler_params=pltpu.CompilerParams(
            collective_id=0, has_side_effects=True, vmem_limit_bytes=56 * 2**20
        ),
        name="wavefields",
    )(*operands)
    return pl.pallas_call(
        publish,
        out_shape=[jax.ShapeDtypeStruct(m.shape, m.dtype) for m in made],
        in_specs=[vmem] * len(made),
        out_specs=[vmem] * len(made),
        compiler_params=pltpu.CompilerParams(vmem_limit_bytes=4 * 2**20),
        name="publish",
    )(*made)


def solution(mesh):
    sizes = tuple(mesh.shape[axis] for axis in AXES)
    field = P(None, ("shot", "inline"), "xline", "depth")
    cell = P("inline", "xline", "depth")
    return jax.shard_map(
        functools.partial(per_device, sizes),
        mesh=mesh,
        in_specs=(
            field, field, field, field,
            cell, cell, cell, cell, cell,
            P(), P(), P("shot"), P("shot"), P("shot"), P(None, "shot"),
        ),
        out_specs=(field, field, P(("shot", "inline"), "xline", "depth"), P(None, "shot")),
        check_vma=False,
    )
```

```python
import functools

import jax
import jax.numpy as jnp
from jax import lax
from jax.experimental import pallas as pl
from jax.experimental.pallas import tpu as pltpu
from jax.sharding import PartitionSpec as P

STEPS = 4
MESH = pl.DeviceIdType.MESH
AXES = ("inline", "xline", "depth")
LANES = 128
TOP = 8

DIRECTIONS = [(a, b) for a in (-1, 0, 1) for b in (-1, 0, 1) if (a, b) != (0, 0)]
SIDES = [d for d in DIRECTIONS if d[0] == 0]
FACES = [d for d in DIRECTIONS if d[0] != 0]


def split_by(values, size):
    if size & (size - 1) == 0:
        return values >> (size.bit_length() - 1), values & (size - 1)
    quotient = lax.div(values, jnp.int32(size))
    return quotient, values - quotient * size


def two_parts(values):
    high = values.astype(jnp.bfloat16)
    return high, (values - high.astype(jnp.float32)).astype(jnp.bfloat16)


def kernel(
    sizes,
    forward_now,
    forward_before,
    adjoint_now,
    adjoint_before,
    courant,
    epsilon,
    delta,
    tilt_class,
    azimuth_class,
    tilt_given,
    azimuth_given,
    source_given,
    wavelet_given,
    cells_given,
    data_given,
    forward_out,
    adjoint_out,
    image_out,
    traces_out,
    fields,
    model,
    classes,
    factors,
    zdiff,
    zsum,
    image,
    tilt_table,
    azimuth_table,
    source_cell,
    wavelet,
    receiver_cells,
    receiver_data,
    hot_row,
    hot_lane,
    spread,
    terms,
    trace_own,
    trace_got,
    trace_all,
    load_sem,
    small_sem,
    ship_recv,
    first_recv,
    halo_send,
    halo_recv,
    trace_send,
    trace_recv,
    terms_send,
    terms_recv,
    go_sem,
    result_send,
    result_recv,
):
    n_in, n_x, n_d = sizes
    _, cx, cy, cz = forward_now.shape
    nrec = cells_given.shape[1]
    groups = cy // 8
    here = tuple(lax.axis_index(axis) for axis in AXES)
    rows = slice(TOP, TOP + cy)
    up = slice(TOP - 1, TOP + cy - 1)
    down = slice(TOP + 1, TOP + cy + 1)
    top = n_d - 1
    leader = here[2] == top

    def present(direction):
        ok = None
        for at, step, size in zip(here, direction, sizes):
            if step == 0:
                continue
            this = (at < size - 1) if step > 0 else (at > 0)
            ok = this if ok is None else jnp.logical_and(ok, this)
        return ok

    def target(direction, depth):
        place = {axis: at + step for axis, at, step in zip(AXES, here, direction) if step != 0}
        return {**place, "depth": depth}

    def opposite(d):
        return tuple(-step for step in d)

    live = [d for d in DIRECTIONS if all(s == 0 or n > 1 for s, n in zip(d, sizes))]
    peers = [(a, b) for a in range(n_in) for b in range(n_x) if (a, b) != (0, 0)]

    def peer(k):
        return {
            "inline": lax.rem(here[0] + peers[k][0], n_in),
            "xline": lax.rem(here[1] + peers[k][1], n_x),
        }

    def at_depth(depth):
        return {"depth": depth}

    inputs = [
        (forward_now, lambda t: fields.at[1, 0, :, pl.ds(1, cx), t, pl.ds(TOP, cy)]),
        (courant, lambda t: model.at[0, :, t]),
        (epsilon, lambda t: model.at[1, :, t]),
        (delta, lambda t: model.at[2, :, t]),
        (tilt_class, lambda t: classes.at[0, :, t]),
        (azimuth_class, lambda t: classes.at[1, :, t]),
        (forward_before, lambda t: fields.at[0, 0, :, pl.ds(1, cx), t, pl.ds(TOP, cy)]),
        (adjoint_now, lambda t: fields.at[1, 1, :, pl.ds(1, cx), t, pl.ds(TOP, cy)]),
        (adjoint_before, lambda t: fields.at[0, 1, :, pl.ds(1, cx), t, pl.ds(TOP, cy)]),
    ]

    nows = (0, 7)

    def load(number, t):
        source, place = inputs[number]
        return pltpu.make_async_copy(source, place(t), load_sem.at[number])

    smalls = [
        (cells_given, receiver_cells),
        (data_given, receiver_data),
        (tilt_given, tilt_table),
        (azimuth_given, azimuth_table),
        (source_given, source_cell),
        (wavelet_given, wavelet),
    ]

    def small(number):
        source, place = smalls[number]
        return pltpu.make_async_copy(source, place, small_sem.at[number])

    def ship(number, t):
        source, place = inputs[number]
        return pltpu.make_async_remote_copy(
            src_ref=source,
            dst_ref=place(t),
            send_sem=load_sem.at[number],
            recv_sem=ship_recv.at[t, number],
            device_id=at_depth(top),
            device_id_type=MESH,
        )

    def wait_input(number):
        if number not in nows:
            load(number, top).wait()
        for t in range(top):
            ship(number, t).wait_recv()

    def edge(step, size, first):
        if step == 0:
            return pl.ds(first, size)
        return pl.ds(first + size - 1 if step > 0 else first, 1)

    def beyond(step, size, first):
        if step == 0:
            return pl.ds(first, size)
        return pl.ds(first - 1 if step > 0 else first + size, 1)

    def first_copy(d, system, t, early):
        return pltpu.make_async_remote_copy(
            src_ref=fields.at[1, system, :, edge(d[0], cx, 1), t, edge(d[1], cy, TOP)],
            dst_ref=fields.at[1, system, :, beyond(d[0], cx, 1), t, beyond(d[1], cy, TOP)],
            send_sem=halo_send.at[system, DIRECTIONS.index(d)],
            recv_sem=(first_recv.at[t] if early else halo_recv.at[0]).at[
                system, DIRECTIONS.index(d)
            ],
            device_id=target(d, top),
            device_id_type=MESH,
        )

    def halo_copy(d, s, system):
        return pltpu.make_async_remote_copy(
            src_ref=fields.at[s + 1, system, :, edge(d[0], cx, 1), :, edge(d[1], cy, TOP)],
            dst_ref=fields.at[s + 1, system, :, beyond(d[0], cx, 1), :, beyond(d[1], cy, TOP)],
            send_sem=halo_send.at[system, DIRECTIONS.index(d)],
            recv_sem=halo_recv.at[s % 2, system, DIRECTIONS.index(d)],
            device_id=target(d, top),
            device_id_type=MESH,
        )

    def trace_copy(late, k):
        steps = pl.ds(STEPS - 1, 1) if late else pl.ds(0, STEPS - 1)
        return pltpu.make_async_remote_copy(
            src_ref=trace_own.at[steps],
            dst_ref=trace_got.at[k, steps],
            send_sem=trace_send.at[late, k],
            recv_sem=trace_recv.at[late, k],
            device_id=peer(k),
            device_id_type=MESH,
        )

    results = [
        (lambda t: fields.at[STEPS + 1, 0, :, pl.ds(1, cx), t, pl.ds(TOP, cy)], forward_out),
        (lambda t: fields.at[STEPS + 1, 1, :, pl.ds(1, cx), t, pl.ds(TOP, cy)], adjoint_out),
        (lambda t: image.at[t], image_out),
        (lambda t: trace_all, traces_out),
    ]

    def result_copy(number, t):
        source, place = results[number]
        return pltpu.make_async_remote_copy(
            src_ref=source(t),
            dst_ref=place,
            send_sem=result_send.at[number, t],
            recv_sem=result_recv.at[number],
            device_id=at_depth(t),
            device_id_type=MESH,
        )

    def give_result(number):
        for t in range(top):
            result_copy(number, t).start()

    barrier = pltpu.get_barrier_semaphore()

    def greet(place):
        pl.semaphore_signal(barrier, inc=1, device_id=place, device_id_type=MESH)

    def send_first(t, system, early):
        for d in sorted(live, key=lambda d: (d[0] == 0, d[1] != 0)):

            @pl.when(present(d))
            def _(d=d):
                first_copy(d, system, t, early).start()

    def drain_first(t, system, early):
        for d in live:

            @pl.when(present(d))
            def _(d=d):
                first_copy(d, system, t, early).wait_send()

    def clear(d):
        for s in range(STEPS):
            for system in range(2):
                place = fields.at[
                    s + 1, system, :, beyond(d[0], cx, 1), :, beyond(d[1], cy, TOP)
                ]
                place[...] = jnp.zeros(place.shape, jnp.float32)

    def clear_absent():
        for d in DIRECTIONS:
            if d not in live:
                clear(d)
            else:

                @pl.when(jnp.logical_not(present(opposite(d))))
                def _(d=d):
                    clear(d)

    def send(s, system, which):
        for d in which:
            if d in live:

                @pl.when(present(d))
                def _(d=d):
                    halo_copy(d, s, system).start()

    def receive(s, system, which):
        for d in which:
            if d in live:

                @pl.when(present(opposite(d)))
                def _(d=d):
                    if s == 0:
                        for t in range(n_d):
                            first_copy(d, system, t, t < top).wait_recv()
                    else:
                        halo_copy(d, s, system).wait_recv()

    def drain(s, system):
        if s == 0:
            drain_first(top, system, False)
            return
        for d in live:

            @pl.when(present(d))
            def _(d=d):
                halo_copy(d, s, system).wait_send()

    lane = lax.broadcasted_iota(jnp.int32, (8, LANES), 1)
    first_lane, last_lane = lane == 0, lane == LANES - 1

    def along_depth(s, system, f, plane, row):
        tiles = [fields[s + 1, system, f, plane, t, row : row + 8, :] for t in range(n_d)]
        right = [pltpu.roll(tile, 1, 1) for tile in tiles]
        left = [pltpu.roll(tile, LANES - 1, 1) for tile in tiles]
        before = [
            jnp.where(first_lane, right[t - 1] if t > 0 else 0.0, right[t]) for t in range(n_d)
        ]
        after = [
            jnp.where(last_lane, left[t + 1] if t < top else 0.0, left[t]) for t in range(n_d)
        ]
        return before, after

    def own_depth(s, system):
        for f in range(2):
            for i in range(cx):
                for r in range(groups):
                    before, after = along_depth(s, system, f, i + 1, TOP + 8 * r)
                    for t in range(n_d):
                        at = slice(TOP + 8 * r, TOP + 8 * r + 8)
                        zdiff[system, f, i + 1, t, at, :] = after[t] - before[t]
                        zsum[system, f, i, t, 8 * r : 8 * r + 8, :] = after[t] + before[t]

    def side_depth(s, system):
        for f in range(2):
            for i in range(cx):
                for row in (0, TOP + cy):
                    before, after = along_depth(s, system, f, i + 1, row)
                    for t in range(n_d):
                        zdiff[system, f, i + 1, t, row : row + 8, :] = after[t] - before[t]

    def face_depth(s, system, plane):
        for f in range(2):
            for r in range(groups):
                before, after = along_depth(s, system, f, plane, TOP + 8 * r)
                for t in range(n_d):
                    at = slice(TOP + 8 * r, TOP + 8 * r + 8)
                    zdiff[system, f, plane, t, at, :] = after[t] - before[t]

    outer = sorted({0, cx - 1})
    inner = [i for i in range(cx) if i not in outer]

    def advance(s, system, i):
        for t in range(n_d):
            axial = []
            lap = None
            doubled = []
            for f in range(2):
                now = fields.at[s + 1, system, f]
                slope = zdiff.at[system, f]
                twice = 2.0 * now[i + 1, t, rows, :]
                doubled.append(twice)
                dxx = now[i + 2, t, rows, :] + now[i, t, rows, :] - twice
                dyy = now[i + 1, t, down, :] + now[i + 1, t, up, :] - twice
                dzz = zsum[system, f, i, t] - twice
                dxy = (
                    now[i + 2, t, down, :]
                    - now[i + 2, t, up, :]
                    - now[i, t, down, :]
                    + now[i, t, up, :]
                )
                dxz = slope[i + 2, t, rows, :] - slope[i, t, rows, :]
                dyz = slope[i + 1, t, down, :] - slope[i + 1, t, up, :]
                axial.append(
                    factors[3, i, t] * dxx
                    + factors[4, i, t] * dyy
                    + factors[5, i, t] * dzz
                    + factors[6, i, t] * dxy
                    + factors[7, i, t] * dxz
                    + factors[8, i, t] * dyz
                )
                if f == 0:
                    lap = dxx + dyy + dzz
            plane_part = lap - axial[0]
            along = factors[2, i, t] * axial[1]
            if system == 0:
                row_at = lax.broadcasted_iota(jnp.int32, (cy, LANES), 0)
                lane_at = lax.broadcasted_iota(jnp.int32, (cy, LANES), 1)
                cell = (
                    (here[0] * cx + i) * (n_x * cy) + here[1] * cy + row_at
                ) * (n_d * cz) + t * cz + lane_at
                added = jnp.where(cell == source_cell[0], wavelet[s], 0.0)
            else:
                added = terms[s, i, t]
            new = []
            for f in range(2):
                value = (
                    doubled[f]
                    - fields[s, system, f, i + 1, t, rows, :]
                    + factors[f, i, t] * plane_part
                    + along
                    + added
                )
                fields[s + 2, system, f, i + 1, t, rows, :] = value
                new.append(value)
            if system == 1:
                product = (
                    fields[s + 2, 0, 0, i + 1, t, rows, :] * new[0]
                    + fields[s + 2, 0, 1, i + 1, t, rows, :] * new[1]
                )
                if s > 0:
                    product = image[t, i] + product
                if s == STEPS - 1 and t == top:
                    image_out[i] = product
                else:
                    image[t, i] = product
            if s == STEPS - 1 and t == top:
                out = forward_out if system == 0 else adjoint_out
                out[0, i] = new[0]
                out[1, i] = new[1]

    def coefficients():
        tilt_sine, tilt_cosine = jnp.sin(tilt_table[...]), jnp.cos(tilt_table[...])
        turn_sine, turn_cosine = jnp.sin(azimuth_table[...]), jnp.cos(azimuth_table[...])

        def spread_out(values):
            wide_table = jnp.zeros((8, LANES), jnp.float32)
            for k in range(values.shape[1]):
                wide_table = jnp.where(
                    lane == k, jnp.broadcast_to(values[:, k : k + 1], (8, LANES)), wide_table
                )
            return wide_table

        tilt_tables = [spread_out(v) for v in (tilt_sine, tilt_cosine)]
        turn_tables = [spread_out(v) for v in (turn_cosine, turn_sine)]

        def look(which, i, t, tables):
            found = [[] for _ in tables]
            for r in range(groups):
                chosen = classes[which, i, t, 8 * r : 8 * r + 8, :]
                for table, parts in zip(tables, found):
                    parts.append(jnp.take_along_axis(table, chosen, axis=1))
            return [jnp.concatenate(parts, axis=0) for parts in found]

        for i in range(cx):
            for t in range(n_d):
                sine, third = look(0, i, t, tilt_tables)
                turned, across = look(1, i, t, turn_tables)
                first, second = sine * turned, sine * across
                base = model[0, i, t]
                factors[0, i, t] = base * (1.0 + 2.0 * model[1, i, t])
                factors[1, i, t] = base * (1.0 + 2.0 * model[2, i, t])
                factors[2, i, t] = base
                factors[3, i, t] = first * first
                factors[4, i, t] = second * second
                factors[5, i, t] = third * third
                factors[6, i, t] = 0.5 * first * second
                factors[7, i, t] = 0.5 * first * third
                factors[8, i, t] = 0.5 * second * third

    volume = cx * cy
    wide = n_d * cz

    def receivers():
        cells = receiver_cells[...]
        upper, depth_at = split_by(cells, wide)
        inline_at, xline_at = split_by(upper, n_x * cy)
        inline_at = inline_at - here[0] * cx
        xline_at = xline_at - here[1] * cy
        inside = (inline_at >= 0) & (inline_at < cx) & (xline_at >= 0) & (xline_at < cy)
        row_of = jnp.where(inside, inline_at * cy + xline_at, -1)
        for start in range(0, volume, 16):
            row_at = start + lax.broadcasted_iota(jnp.int32, (16, nrec), 0)
            match = row_at == jnp.broadcast_to(row_of, (16, nrec))
            hot_row[start : start + 16, :] = jnp.where(match, 1.0, 0.0)
        for start in range(0, wide, 16):
            lane_at = start + lax.broadcasted_iota(jnp.int32, (16, nrec), 0)
            match = lane_at == jnp.broadcast_to(depth_at, (16, nrec))
            hot_lane[start : start + 16, :] = jnp.where(match, 1.0, 0.0).astype(jnp.bfloat16)

    def injection(s):
        for number, part in enumerate(two_parts(receiver_data[s : s + 1, :])):
            spread[number * volume : (number + 1) * volume, :] = hot_row[...].astype(
                jnp.bfloat16
            ) * jnp.broadcast_to(part, (volume, nrec))
        got = lax.dot_general(
            spread[...],
            hot_lane[...],
            (((1,), (1,)), ((), ())),
            preferred_element_type=jnp.float32,
        )
        total = got[:volume] + got[volume:]
        for i in range(cx):
            for t in range(n_d):
                terms[s, i, t] = total[i * cy : (i + 1) * cy, t * cz : (t + 1) * cz]

    def sample(s):
        tiles = [
            jnp.concatenate(
                [fields[s + 2, 0, 0, i + 1, t, rows, :] for i in range(cx)], axis=0
            )
            for t in range(n_d)
        ]
        split = [two_parts(tile) for tile in tiles]
        parts = jnp.concatenate(
            [
                jnp.concatenate([split[t][part] for t in range(n_d)], axis=1)
                for part in range(2)
            ],
            axis=0,
        )
        picked = jnp.dot(parts, hot_lane[...], preferred_element_type=jnp.float32)
        picked = picked[:volume] + picked[volume:]
        trace_own[s] = jnp.sum(picked * hot_row[...], axis=0, keepdims=True)

    def share(late):
        for k in range(len(peers)):
            trace_copy(late, k).start()

    def finish_trace(late):
        for k in range(len(peers)):
            trace_copy(late, k).wait_recv()
        for s in [STEPS - 1] if late else range(STEPS - 1):
            total = trace_own[s]
            for k in range(len(peers)):
                total = total + trace_got[k, s]
            traces_out[s : s + 1, :] = total
            trace_all[s : s + 1, :] = total

    def terms_copy(s):
        return pltpu.make_async_remote_copy(
            src_ref=terms.at[s],
            dst_ref=terms.at[s],
            send_sem=terms_send.at[s],
            recv_sem=terms_recv.at[s],
            device_id=at_depth(top),
            device_id_type=MESH,
        )

    nearby = max(n_in, n_x) <= STEPS
    neighbours = jnp.int32(0)
    for d in live:
        neighbours = neighbours + jnp.where(present(d), 1, 0)

    @pl.when(jnp.logical_not(leader))
    def _():
        greet(at_depth(top))
        for number in nows:
            load(number, here[2]).start()
        for number in (0, 1):
            small(number).start()
        pl.semaphore_wait(barrier, 1)
        for number in range(1, 7):
            ship(number, here[2]).start()
        for number in nows:
            load(number, here[2]).wait()
        pl.semaphore_wait(go_sem, 1)
        send_first(here[2], 0, True)
        ship(0, here[2]).start()
        send_first(here[2], 1, True)
        for number in (7, 8):
            ship(number, here[2]).start()
        for number in (0, 1):
            small(number).wait()

        @pl.when(here[2] == 0)
        def _():
            receivers()
            for s in range(STEPS):
                injection(s)
                terms_copy(s).start()
            for s in range(STEPS):
                terms_copy(s).wait_send()

        for number in range(len(inputs)):
            ship(number, here[2]).wait_send()
        for system in range(2):
            drain_first(here[2], system, True)
        for number in range(len(results)):
            result_copy(number, here[2]).wait_recv()

    @pl.when(leader)
    def _():
        if nearby:
            for d in sorted(live, key=lambda d: d[0] * d[1] != 0):

                @pl.when(present(d))
                def _(d=d):
                    greet(target(d, top))

        else:
            for k in range(len(peers)):
                greet(peer(k))
        for t in range(top):
            greet(at_depth(t))
        for number in nows:
            load(number, top).start()
        for number in range(len(smalls)):
            small(number).start()
        for number in range(len(inputs)):
            if number not in nows:
                load(number, top).start()
        pl.semaphore_wait(barrier, (neighbours if nearby else len(peers)) + top)
        for t in range(top):
            pl.semaphore_signal(
                go_sem, inc=1, device_id=at_depth(t), device_id_type=MESH
            )
        for system in range(2):
            load(nows[system], top).wait()
            send_first(top, system, False)
        clear_absent()
        for number in range(len(smalls)):
            small(number).wait()
        for number in range(1, 6):
            wait_input(number)
        coefficients()
        wait_input(0)
        own_depth(0, 0)
        receivers()
        wait_input(6)
        if top == 0:
            for s in range(STEPS):
                injection(s)
        for s in range(STEPS):
            for system in range(2):
                if s == 0 and system == 1:
                    wait_input(7)
                    own_depth(0, 1)
                    wait_input(8)
                if system == 1 and top > 0:
                    terms_copy(s).wait_recv()
                drain(s, system)
                receive(s, system, SIDES)
                side_depth(s, system)
                for i in inner:
                    advance(s, system, i)
                if cx > 1:
                    for i, side in ((0, 1), (cx - 1, -1)):
                        receive(s, system, [d for d in FACES if d[0] == side])
                        face_depth(s, system, 0 if side > 0 else cx + 1)
                        advance(s, system, i)
                        if s < STEPS - 1:
                            send(s + 1, system, [d for d in FACES if d[0] == -side])
                else:
                    receive(s, system, FACES)
                    for plane in (0, cx + 1):
                        face_depth(s, system, plane)
                    advance(s, system, 0)
                    if s < STEPS - 1:
                        send(s + 1, system, FACES)
                if s < STEPS - 1:
                    send(s + 1, system, SIDES)
                    own_depth(s + 1, system)
                if system == 0:
                    sample(s)
                    if s == STEPS - 1:
                        share(1)
                elif s == STEPS - 2:
                    share(0)
                if s == STEPS - 1:
                    give_result(system)
        give_result(2)
        for late in range(2):
            finish_trace(late)
        give_result(3)
        for late in range(2):
            for k in range(len(peers)):
                trace_copy(late, k).wait_send()
        for number in range(len(results)):
            for t in range(top):
                result_copy(number, t).wait_send()


def publish(*refs):
    half = len(refs) // 2
    for source, place in zip(refs[:half], refs[half:]):
        place[...] = source[...]


def per_device(sizes, *operands):
    shapes = [operand.shape for operand in operands]
    _, cx, cy, cz = shapes[0]
    nrec = shapes[13][0]
    n_in, n_x, n_d = sizes
    operands = list(operands)
    for which in (9, 10, 13):
        operands[which] = operands[which].reshape(1, -1)
    f32, bf16 = jnp.float32, jnp.bfloat16
    padded = cy + 2 * TOP
    chips = n_in * n_x
    count = len(DIRECTIONS)
    others = max(n_d - 1, 1)
    dma = pltpu.SemaphoreType.DMA
    scratch = [
        pltpu.VMEM((STEPS + 2, 2, 2, cx + 2, n_d, padded, cz), f32),
        pltpu.VMEM((3, cx, n_d, cy, cz), f32),
        pltpu.VMEM((2, cx, n_d, cy, cz), jnp.int32),
        pltpu.VMEM((9, cx, n_d, cy, cz), f32),
        pltpu.VMEM((2, 2, cx + 2, n_d, padded, cz), f32),
        pltpu.VMEM((2, 2, cx, n_d, cy, cz), f32),
        pltpu.VMEM((n_d, cx, cy, cz), f32),
        pltpu.VMEM(operands[9].shape, f32),
        pltpu.VMEM(operands[10].shape, f32),
        pltpu.SMEM(shapes[11], jnp.int32),
        pltpu.SMEM(shapes[12], f32),
        pltpu.VMEM(operands[13].shape, jnp.int32),
        pltpu.VMEM(shapes[14], f32),
        pltpu.VMEM((cx * cy, nrec), f32),
        pltpu.VMEM((n_d * cz, nrec), bf16),
        pltpu.VMEM((2 * cx * cy, nrec), bf16),
        pltpu.VMEM((STEPS, cx, n_d, cy, cz), f32),
        pltpu.VMEM((STEPS, 1, nrec), f32),
        pltpu.VMEM((chips, STEPS, 1, nrec), f32),
        pltpu.VMEM((STEPS, nrec), f32),
        dma((9,)),
        dma((6,)),
        dma((others, 9)),
        dma((others, 2, count)),
        dma((2, count)),
        dma((2, 2, count)),
        dma((2, max(chips - 1, 1))),
        dma((2, max(chips - 1, 1))),
        dma((STEPS,)),
        dma((STEPS,)),
        pltpu.SemaphoreType.REGULAR,
        dma((4, others)),
        dma((4,)),
    ]
    vmem = pl.BlockSpec(memory_space=pltpu.VMEM)
    anywhere = pl.BlockSpec(memory_space=pl.ANY)
    made = pl.pallas_call(
        functools.partial(kernel, sizes),
        out_shape=(
            pltpu.VMEM((2, cx, cy, cz), f32),
            pltpu.VMEM((2, cx, cy, cz), f32),
            pltpu.VMEM((cx, cy, cz), f32),
            pltpu.VMEM((STEPS, nrec), f32),
        ),
        in_specs=[anywhere] * len(operands),
        out_specs=(vmem, vmem, vmem, vmem),
        scratch_shapes=scratch,
        compiler_params=pltpu.CompilerParams(
            collective_id=0, has_side_effects=True, vmem_limit_bytes=56 * 2**20
        ),
        name="wavefields",
    )(*operands)
    return pl.pallas_call(
        publish,
        out_shape=[jax.ShapeDtypeStruct(m.shape, m.dtype) for m in made],
        in_specs=[vmem] * len(made),
        out_specs=[vmem] * len(made),
        compiler_params=pltpu.CompilerParams(vmem_limit_bytes=4 * 2**20),
        name="publish",
    )(*made)


def solution(mesh):
    sizes = tuple(mesh.shape[axis] for axis in AXES)
    field = P(None, ("shot", "inline"), "xline", "depth")
    cell = P("inline", "xline", "depth")
    return jax.shard_map(
        functools.partial(per_device, sizes),
        mesh=mesh,
        in_specs=(
            field, field, field, field,
            cell, cell, cell, cell, cell,
            P(), P(), P("shot"), P("shot"), P("shot"), P(None, "shot"),
        ),
        out_specs=(field, field, P(("shot", "inline"), "xline", "depth"), P(None, "shot")),
        check_vma=False,
    )
```

```python
import functools

import jax
import jax.numpy as jnp
from jax import lax
from jax.experimental import pallas as pl
from jax.experimental.pallas import tpu as pltpu
from jax.sharding import PartitionSpec as P

STEPS = 4
MESH = pl.DeviceIdType.MESH
AXES = ("inline", "xline", "depth")
LANES = 128
TOP = 8

DIRECTIONS = [(a, b) for a in (-1, 0, 1) for b in (-1, 0, 1) if (a, b) != (0, 0)]
SIDES = [d for d in DIRECTIONS if d[0] == 0]
FACES = [d for d in DIRECTIONS if d[0] != 0]


def split_by(values, size):
    if size & (size - 1) == 0:
        return values >> (size.bit_length() - 1), values & (size - 1)
    quotient = lax.div(values, jnp.int32(size))
    return quotient, values - quotient * size


def two_parts(values):
    high = values.astype(jnp.bfloat16)
    return high, (values - high.astype(jnp.float32)).astype(jnp.bfloat16)


def kernel(
    sizes,
    forward_now,
    forward_before,
    adjoint_now,
    adjoint_before,
    courant,
    epsilon,
    delta,
    tilt_class,
    azimuth_class,
    tilt_given,
    azimuth_given,
    source_given,
    wavelet_given,
    cells_given,
    data_given,
    forward_out,
    adjoint_out,
    image_out,
    traces_out,
    fields,
    model,
    classes,
    factors,
    zdiff,
    zsum,
    image,
    tilt_table,
    azimuth_table,
    source_cell,
    wavelet,
    receiver_cells,
    receiver_data,
    hot_row,
    hot_lane,
    spread,
    terms,
    trace_own,
    trace_got,
    trace_all,
    load_sem,
    small_sem,
    ship_recv,
    halo_send,
    halo_recv,
    trace_send,
    trace_recv,
    terms_send,
    terms_recv,
    go_sem,
    result_send,
    result_recv,
):
    n_in, n_x, n_d = sizes
    _, cx, cy, cz = forward_now.shape
    nrec = cells_given.shape[1]
    groups = cy // 8
    here = tuple(lax.axis_index(axis) for axis in AXES)
    rows = slice(TOP, TOP + cy)
    up = slice(TOP - 1, TOP + cy - 1)
    down = slice(TOP + 1, TOP + cy + 1)
    top = n_d - 1
    leader = here[2] == top

    def present(direction):
        ok = None
        for at, step, size in zip(here, direction, sizes):
            if step == 0:
                continue
            this = (at < size - 1) if step > 0 else (at > 0)
            ok = this if ok is None else jnp.logical_and(ok, this)
        return ok

    def target(direction, depth):
        place = {axis: at + step for axis, at, step in zip(AXES, here, direction) if step != 0}
        return {**place, "depth": depth}

    def opposite(d):
        return tuple(-step for step in d)

    live = [d for d in DIRECTIONS if all(s == 0 or n > 1 for s, n in zip(d, sizes))]
    peers = [(a, b) for a in range(n_in) for b in range(n_x) if (a, b) != (0, 0)]

    def peer(k):
        return {
            "inline": lax.rem(here[0] + peers[k][0], n_in),
            "xline": lax.rem(here[1] + peers[k][1], n_x),
        }

    def at_depth(depth):
        return {"depth": depth}

    planes, lines = pl.ds(1, cx), pl.ds(TOP, cy)
    before, now = (forward_before, adjoint_before), (forward_now, adjoint_now)

    def group_place(group, t):
        if group == "model":
            return model.at[:, :, t]
        if group == "classes":
            return classes.at[:, :, t]
        if group == "before":
            return fields.at[0, :, :, planes, t, lines]
        return fields.at[pl.ds(0, 2), group, :, planes, t, lines]

    model_copies = [(array, model, n) for n, array in enumerate((courant, epsilon, delta))]
    class_copies = [(array, classes, n) for n, array in enumerate((tilt_class, azimuth_class))]

    def members(group, t):
        if group in ("model", "classes"):
            return [
                (array, place.at[n, :, t])
                for array, place, n in (model_copies if group == "model" else class_copies)
            ]
        if group == "before":
            return [
                (before[system], fields.at[0, system, :, planes, t, lines])
                for system in range(2)
            ]
        return [
            (now[group], fields.at[1, group, :, planes, t, lines]),
            (before[group], fields.at[0, group, :, planes, t, lines]),
        ]

    def load_now(system, t):
        return pltpu.make_async_copy(
            now[system], fields.at[1, system, :, planes, t, lines], load_sem.at[system]
        )

    loaded = {"model": 2, "classes": 3, "before": 4}
    shipped = {"model": 2, "classes": 3, 0: 4, 1: 0}
    landed = {"model": 0, "classes": 1, 0: 2, 1: 3}

    def start_load(group):
        for source, place in members(group, top):
            pltpu.make_async_copy(source, place, load_sem.at[loaded[group]]).start()

    def wait_load(group):
        place = group_place(group, top)
        pltpu.make_async_copy(place, place, load_sem.at[loaded[group]]).wait()

    def ship(group, t, source, place):
        return pltpu.make_async_remote_copy(
            src_ref=source,
            dst_ref=place,
            send_sem=load_sem.at[shipped[group]],
            recv_sem=ship_recv.at[t, landed[group]],
            device_id=at_depth(top),
            device_id_type=MESH,
        )

    def start_ship(group, t):
        for source, place in members(group, t):
            ship(group, t, source, place).start()

    def whole_ship(group, t):
        place = group_place(group, t)
        return ship(group, t, place, place)

    def wait_ship(group):
        for t in range(top):
            whole_ship(group, t).wait_recv()

    smalls = [
        (cells_given, receiver_cells),
        (data_given, receiver_data),
        (tilt_given, tilt_table),
        (azimuth_given, azimuth_table),
        (source_given, source_cell),
        (wavelet_given, wavelet),
    ]

    def small(number):
        source, place = smalls[number]
        return pltpu.make_async_copy(source, place, small_sem.at[number])

    def edge(step, size, first):
        if step == 0:
            return pl.ds(first, size)
        return pl.ds(first + size - 1 if step > 0 else first, 1)

    def beyond(step, size, first):
        if step == 0:
            return pl.ds(first, size)
        return pl.ds(first - 1 if step > 0 else first + size, 1)

    def first_copy(d, system, t):
        return pltpu.make_async_remote_copy(
            src_ref=fields.at[1, system, :, edge(d[0], cx, 1), t, edge(d[1], cy, TOP)],
            dst_ref=fields.at[1, system, :, beyond(d[0], cx, 1), t, beyond(d[1], cy, TOP)],
            send_sem=halo_send.at[system, DIRECTIONS.index(d)],
            recv_sem=halo_recv.at[0, system, DIRECTIONS.index(d)],
            device_id=target(d, top),
            device_id_type=MESH,
        )

    def halo_copy(d, s, system):
        return pltpu.make_async_remote_copy(
            src_ref=fields.at[s + 1, system, :, edge(d[0], cx, 1), :, edge(d[1], cy, TOP)],
            dst_ref=fields.at[s + 1, system, :, beyond(d[0], cx, 1), :, beyond(d[1], cy, TOP)],
            send_sem=halo_send.at[system, DIRECTIONS.index(d)],
            recv_sem=halo_recv.at[s % 2, system, DIRECTIONS.index(d)],
            device_id=target(d, top),
            device_id_type=MESH,
        )

    def trace_copy(late, k):
        steps = pl.ds(STEPS - 1, 1) if late else pl.ds(0, STEPS - 1)
        return pltpu.make_async_remote_copy(
            src_ref=trace_own.at[steps],
            dst_ref=trace_got.at[k, steps],
            send_sem=trace_send.at[late],
            recv_sem=trace_recv.at[late],
            device_id=peer(k),
            device_id_type=MESH,
        )

    results = [
        (lambda t: fields.at[STEPS + 1, 0, :, pl.ds(1, cx), t, pl.ds(TOP, cy)], forward_out),
        (lambda t: fields.at[STEPS + 1, 1, :, pl.ds(1, cx), t, pl.ds(TOP, cy)], adjoint_out),
        (lambda t: image.at[t], image_out),
        (lambda t: trace_all, traces_out),
    ]

    def result_copy(number, t):
        source, place = results[number]
        return pltpu.make_async_remote_copy(
            src_ref=source(t),
            dst_ref=place,
            send_sem=result_send.at[number, t],
            recv_sem=result_recv.at[number],
            device_id=at_depth(t),
            device_id_type=MESH,
        )

    def give_result(number):
        for t in range(top):
            result_copy(number, t).start()

    barrier = pltpu.get_barrier_semaphore()

    def greet(place):
        pl.semaphore_signal(barrier, inc=1, device_id=place, device_id_type=MESH)

    def send_first(t, system):
        for d in sorted(live, key=lambda d: (d[0] == 0, d[1] != 0)):

            @pl.when(present(d))
            def _(d=d):
                first_copy(d, system, t).start()

    def drain_first(t, system):
        for d in live:

            @pl.when(present(d))
            def _(d=d):
                first_copy(d, system, t).wait_send()

    def clear(d):
        for s in range(STEPS):
            for system in range(2):
                place = fields.at[
                    s + 1, system, :, beyond(d[0], cx, 1), :, beyond(d[1], cy, TOP)
                ]
                place[...] = jnp.zeros(place.shape, jnp.float32)

    def clear_absent():
        for d in DIRECTIONS:
            if d not in live:
                clear(d)
            else:

                @pl.when(jnp.logical_not(present(opposite(d))))
                def _(d=d):
                    clear(d)

    def send(s, system, which):
        for d in which:
            if d in live:

                @pl.when(present(d))
                def _(d=d):
                    halo_copy(d, s, system).start()

    def receive(s, system, which):
        for d in which:
            if d in live:

                @pl.when(present(opposite(d)))
                def _(d=d):
                    halo_copy(d, s, system).wait_recv()

    def drain(s, system):
        if s == 0:
            drain_first(top, system)
            return
        for d in live:

            @pl.when(present(d))
            def _(d=d):
                halo_copy(d, s, system).wait_send()

    lane = lax.broadcasted_iota(jnp.int32, (8, LANES), 1)
    first_lane, last_lane = lane == 0, lane == LANES - 1

    def along_depth(s, system, f, plane, row):
        tiles = [fields[s + 1, system, f, plane, t, row : row + 8, :] for t in range(n_d)]
        right = [pltpu.roll(tile, 1, 1) for tile in tiles]
        left = [pltpu.roll(tile, LANES - 1, 1) for tile in tiles]
        before = [
            jnp.where(first_lane, right[t - 1] if t > 0 else 0.0, right[t]) for t in range(n_d)
        ]
        after = [
            jnp.where(last_lane, left[t + 1] if t < top else 0.0, left[t]) for t in range(n_d)
        ]
        return before, after

    def own_depth(s, system):
        for f in range(2):
            for i in range(cx):
                for r in range(groups):
                    before, after = along_depth(s, system, f, i + 1, TOP + 8 * r)
                    for t in range(n_d):
                        at = slice(TOP + 8 * r, TOP + 8 * r + 8)
                        zdiff[system, f, i + 1, t, at, :] = after[t] - before[t]
                        zsum[system, f, i, t, 8 * r : 8 * r + 8, :] = after[t] + before[t]

    def side_depth(s, system):
        for f in range(2):
            for i in range(cx):
                for row in (0, TOP + cy):
                    before, after = along_depth(s, system, f, i + 1, row)
                    for t in range(n_d):
                        zdiff[system, f, i + 1, t, row : row + 8, :] = after[t] - before[t]

    def face_depth(s, system, plane):
        for f in range(2):
            for r in range(groups):
                before, after = along_depth(s, system, f, plane, TOP + 8 * r)
                for t in range(n_d):
                    at = slice(TOP + 8 * r, TOP + 8 * r + 8)
                    zdiff[system, f, plane, t, at, :] = after[t] - before[t]

    outer = sorted({0, cx - 1})
    inner = [i for i in range(cx) if i not in outer]

    def advance(s, system, i):
        for t in range(n_d):
            axial = []
            lap = None
            doubled = []
            for f in range(2):
                now = fields.at[s + 1, system, f]
                slope = zdiff.at[system, f]
                twice = 2.0 * now[i + 1, t, rows, :]
                doubled.append(twice)
                dxx = now[i + 2, t, rows, :] + now[i, t, rows, :] - twice
                dyy = now[i + 1, t, down, :] + now[i + 1, t, up, :] - twice
                dzz = zsum[system, f, i, t] - twice
                dxy = (
                    now[i + 2, t, down, :]
                    - now[i + 2, t, up, :]
                    - now[i, t, down, :]
                    + now[i, t, up, :]
                )
                dxz = slope[i + 2, t, rows, :] - slope[i, t, rows, :]
                dyz = slope[i + 1, t, down, :] - slope[i + 1, t, up, :]
                axial.append(
                    factors[3, i, t] * dxx
                    + factors[4, i, t] * dyy
                    + factors[5, i, t] * dzz
                    + factors[6, i, t] * dxy
                    + factors[7, i, t] * dxz
                    + factors[8, i, t] * dyz
                )
                if f == 0:
                    lap = dxx + dyy + dzz
            plane_part = lap - axial[0]
            along = factors[2, i, t] * axial[1]
            if system == 0:
                row_at = lax.broadcasted_iota(jnp.int32, (cy, LANES), 0)
                lane_at = lax.broadcasted_iota(jnp.int32, (cy, LANES), 1)
                cell = (
                    (here[0] * cx + i) * (n_x * cy) + here[1] * cy + row_at
                ) * (n_d * cz) + t * cz + lane_at
                added = jnp.where(cell == source_cell[0], wavelet[s], 0.0)
            else:
                added = terms[s, i, t]
            new = []
            for f in range(2):
                value = (
                    doubled[f]
                    - fields[s, system, f, i + 1, t, rows, :]
                    + factors[f, i, t] * plane_part
                    + along
                    + added
                )
                fields[s + 2, system, f, i + 1, t, rows, :] = value
                new.append(value)
            if system == 1:
                product = (
                    fields[s + 2, 0, 0, i + 1, t, rows, :] * new[0]
                    + fields[s + 2, 0, 1, i + 1, t, rows, :] * new[1]
                )
                if s > 0:
                    product = image[t, i] + product
                if s == STEPS - 1 and t == top:
                    image_out[i] = product
                else:
                    image[t, i] = product
            if s == STEPS - 1 and t == top:
                out = forward_out if system == 0 else adjoint_out
                out[0, i] = new[0]
                out[1, i] = new[1]

    def coefficients():
        tilt_sine, tilt_cosine = jnp.sin(tilt_table[...]), jnp.cos(tilt_table[...])
        turn_sine, turn_cosine = jnp.sin(azimuth_table[...]), jnp.cos(azimuth_table[...])

        def spread_out(values):
            wide_table = jnp.zeros((8, LANES), jnp.float32)
            for k in range(values.shape[1]):
                wide_table = jnp.where(
                    lane == k, jnp.broadcast_to(values[:, k : k + 1], (8, LANES)), wide_table
                )
            return wide_table

        tilt_tables = [spread_out(v) for v in (tilt_sine, tilt_cosine)]
        turn_tables = [spread_out(v) for v in (turn_cosine, turn_sine)]

        def look(which, i, t, tables):
            found = [[] for _ in tables]
            for r in range(groups):
                chosen = classes[which, i, t, 8 * r : 8 * r + 8, :]
                for table, parts in zip(tables, found):
                    parts.append(jnp.take_along_axis(table, chosen, axis=1))
            return [jnp.concatenate(parts, axis=0) for parts in found]

        for i in range(cx):
            for t in range(n_d):
                sine, third = look(0, i, t, tilt_tables)
                turned, across = look(1, i, t, turn_tables)
                first, second = sine * turned, sine * across
                base = model[0, i, t]
                factors[0, i, t] = base * (1.0 + 2.0 * model[1, i, t])
                factors[1, i, t] = base * (1.0 + 2.0 * model[2, i, t])
                factors[2, i, t] = base
                factors[3, i, t] = first * first
                factors[4, i, t] = second * second
                factors[5, i, t] = third * third
                factors[6, i, t] = 0.5 * first * second
                factors[7, i, t] = 0.5 * first * third
                factors[8, i, t] = 0.5 * second * third

    volume = cx * cy
    wide = n_d * cz

    def receivers():
        cells = receiver_cells[...]
        upper, depth_at = split_by(cells, wide)
        inline_at, xline_at = split_by(upper, n_x * cy)
        inline_at = inline_at - here[0] * cx
        xline_at = xline_at - here[1] * cy
        inside = (inline_at >= 0) & (inline_at < cx) & (xline_at >= 0) & (xline_at < cy)
        row_of = jnp.where(inside, inline_at * cy + xline_at, -1)
        for start in range(0, volume, 16):
            row_at = start + lax.broadcasted_iota(jnp.int32, (16, nrec), 0)
            match = row_at == jnp.broadcast_to(row_of, (16, nrec))
            hot_row[start : start + 16, :] = jnp.where(match, 1.0, 0.0)
        for start in range(0, wide, 16):
            lane_at = start + lax.broadcasted_iota(jnp.int32, (16, nrec), 0)
            match = lane_at == jnp.broadcast_to(depth_at, (16, nrec))
            hot_lane[start : start + 16, :] = jnp.where(match, 1.0, 0.0).astype(jnp.bfloat16)

    def injection(s):
        for number, part in enumerate(two_parts(receiver_data[s : s + 1, :])):
            spread[number * volume : (number + 1) * volume, :] = hot_row[...].astype(
                jnp.bfloat16
            ) * jnp.broadcast_to(part, (volume, nrec))
        got = lax.dot_general(
            spread[...],
            hot_lane[...],
            (((1,), (1,)), ((), ())),
            preferred_element_type=jnp.float32,
        )
        total = got[:volume] + got[volume:]
        for i in range(cx):
            for t in range(n_d):
                terms[s, i, t] = total[i * cy : (i + 1) * cy, t * cz : (t + 1) * cz]

    def sample(s):
        tiles = [
            jnp.concatenate(
                [fields[s + 2, 0, 0, i + 1, t, rows, :] for i in range(cx)], axis=0
            )
            for t in range(n_d)
        ]
        split = [two_parts(tile) for tile in tiles]
        parts = jnp.concatenate(
            [
                jnp.concatenate([split[t][part] for t in range(n_d)], axis=1)
                for part in range(2)
            ],
            axis=0,
        )
        picked = jnp.dot(parts, hot_lane[...], preferred_element_type=jnp.float32)
        picked = picked[:volume] + picked[volume:]
        trace_own[s] = jnp.sum(picked * hot_row[...], axis=0, keepdims=True)

    def share(late):
        for k in range(len(peers)):
            trace_copy(late, k).start()

    def whole_trace(late):
        steps = pl.ds(STEPS - 1, 1) if late else pl.ds(0, STEPS - 1)
        place = trace_got.at[pl.ds(0, len(peers)), steps]
        return pltpu.make_async_remote_copy(
            src_ref=place,
            dst_ref=place,
            send_sem=trace_send.at[late],
            recv_sem=trace_recv.at[late],
            device_id=peer(0),
            device_id_type=MESH,
        )

    def finish_trace(late):
        if peers:
            whole_trace(late).wait_recv()
        for s in [STEPS - 1] if late else range(STEPS - 1):
            total = trace_own[s]
            for k in range(len(peers)):
                total = total + trace_got[k, s]
            traces_out[s : s + 1, :] = total
            trace_all[s : s + 1, :] = total

    def terms_copy(first, count):
        return pltpu.make_async_remote_copy(
            src_ref=terms.at[pl.ds(first, count)],
            dst_ref=terms.at[pl.ds(first, count)],
            send_sem=terms_send,
            recv_sem=terms_recv.at[min(first, 1)],
            device_id=at_depth(top),
            device_id_type=MESH,
        )

    nearby = max(n_in, n_x) <= STEPS
    neighbours = jnp.int32(0)
    for d in live:
        neighbours = neighbours + jnp.where(present(d), 1, 0)

    @pl.when(jnp.logical_not(leader))
    def _():
        greet(at_depth(top))
        for system in range(2):
            load_now(system, here[2]).start()
        for number in (0, 1):
            small(number).start()
        pl.semaphore_wait(barrier, 1)
        for group in ("classes", "model"):
            start_ship(group, here[2])
        for system in range(2):
            load_now(system, here[2]).wait()
        pl.semaphore_wait(go_sem, 1)
        for system in range(2):
            send_first(here[2], system)
            start_ship(system, here[2])
        for number in (0, 1):
            small(number).wait()

        @pl.when(here[2] == 0)
        def _():
            receivers()
            for s in range(STEPS):
                injection(s)
                terms_copy(s, 1).start()
            terms_copy(0, STEPS).wait_send()

        for group in ("classes", "model", 0, 1):
            whole_ship(group, here[2]).wait_send()
        for system in range(2):
            drain_first(here[2], system)
        for number in range(len(results)):
            result_copy(number, here[2]).wait_recv()

    @pl.when(leader)
    def _():
        if nearby:
            for d in sorted(live, key=lambda d: d[0] * d[1] != 0):

                @pl.when(present(d))
                def _(d=d):
                    greet(target(d, top))

        else:
            for k in range(len(peers)):
                greet(peer(k))
        for t in range(top):
            greet(at_depth(t))
        for system in range(2):
            load_now(system, top).start()
        for number in range(len(smalls)):
            small(number).start()
        for group in ("classes", "model", "before"):
            start_load(group)
        pl.semaphore_wait(barrier, (neighbours if nearby else len(peers)) + top)
        for t in range(top):
            pl.semaphore_signal(
                go_sem, inc=1, device_id=at_depth(t), device_id_type=MESH
            )
        for system in range(2):
            load_now(system, top).wait()
            send_first(top, system)
        clear_absent()
        for number in range(len(smalls)):
            small(number).wait()
        for group in ("classes", "model"):
            wait_load(group)
            wait_ship(group)
        coefficients()
        receivers()
        wait_load("before")
        wait_ship(0)
        own_depth(0, 0)
        if top == 0:
            for s in range(STEPS):
                injection(s)
        for s in range(STEPS):
            for system in range(2):
                if s == 0 and system == 1:
                    wait_ship(1)
                    own_depth(0, 1)
                if system == 1 and top > 0 and s < 2:
                    terms_copy(s, STEPS - 1 if s else 1).wait_recv()
                drain(s, system)
                receive(s, system, SIDES)
                side_depth(s, system)
                for i in inner:
                    advance(s, system, i)
                if cx > 1:
                    for i, side in ((0, 1), (cx - 1, -1)):
                        receive(s, system, [d for d in FACES if d[0] == side])
                        face_depth(s, system, 0 if side > 0 else cx + 1)
                        advance(s, system, i)
                        if s < STEPS - 1:
                            send(s + 1, system, [d for d in FACES if d[0] == -side])
                else:
                    receive(s, system, FACES)
                    for plane in (0, cx + 1):
                        face_depth(s, system, plane)
                    advance(s, system, 0)
                    if s < STEPS - 1:
                        send(s + 1, system, FACES)
                if s < STEPS - 1:
                    send(s + 1, system, SIDES)
                    own_depth(s + 1, system)
                if system == 0:
                    sample(s)
                    if s == STEPS - 1:
                        share(1)
                elif s == STEPS - 2:
                    share(0)
                if s == STEPS - 1:
                    give_result(system)
        give_result(2)
        for late in range(2):
            finish_trace(late)
        give_result(3)
        if peers:
            for late in range(2):
                whole_trace(late).wait_send()
        for number in range(len(results)):
            for t in range(top):
                result_copy(number, t).wait_send()


def publish(*refs):
    half = len(refs) // 2
    for source, place in zip(refs[:half], refs[half:]):
        place[...] = source[...]


def per_device(sizes, *operands):
    shapes = [operand.shape for operand in operands]
    _, cx, cy, cz = shapes[0]
    nrec = shapes[13][0]
    n_in, n_x, n_d = sizes
    operands = list(operands)
    for which in (9, 10, 13):
        operands[which] = operands[which].reshape(1, -1)
    f32, bf16 = jnp.float32, jnp.bfloat16
    padded = cy + 2 * TOP
    chips = n_in * n_x
    count = len(DIRECTIONS)
    others = max(n_d - 1, 1)
    dma = pltpu.SemaphoreType.DMA
    scratch = [
        pltpu.VMEM((STEPS + 2, 2, 2, cx + 2, n_d, padded, cz), f32),
        pltpu.VMEM((3, cx, n_d, cy, cz), f32),
        pltpu.VMEM((2, cx, n_d, cy, cz), jnp.int32),
        pltpu.VMEM((9, cx, n_d, cy, cz), f32),
        pltpu.VMEM((2, 2, cx + 2, n_d, padded, cz), f32),
        pltpu.VMEM((2, 2, cx, n_d, cy, cz), f32),
        pltpu.VMEM((n_d, cx, cy, cz), f32),
        pltpu.VMEM(operands[9].shape, f32),
        pltpu.VMEM(operands[10].shape, f32),
        pltpu.SMEM(shapes[11], jnp.int32),
        pltpu.SMEM(shapes[12], f32),
        pltpu.VMEM(operands[13].shape, jnp.int32),
        pltpu.VMEM(shapes[14], f32),
        pltpu.VMEM((cx * cy, nrec), f32),
        pltpu.VMEM((n_d * cz, nrec), bf16),
        pltpu.VMEM((2 * cx * cy, nrec), bf16),
        pltpu.VMEM((STEPS, cx, n_d, cy, cz), f32),
        pltpu.VMEM((STEPS, 1, nrec), f32),
        pltpu.VMEM((chips, STEPS, 1, nrec), f32),
        pltpu.VMEM((STEPS, nrec), f32),
        dma((5,)),
        dma((6,)),
        dma((others, 4)),
        dma((2, count)),
        dma((2, 2, count)),
        dma((2,)),
        dma((2,)),
        dma,
        dma((2,)),
        pltpu.SemaphoreType.REGULAR,
        dma((4, others)),
        dma((4,)),
    ]
    vmem = pl.BlockSpec(memory_space=pltpu.VMEM)
    anywhere = pl.BlockSpec(memory_space=pl.ANY)
    made = pl.pallas_call(
        functools.partial(kernel, sizes),
        out_shape=(
            pltpu.VMEM((2, cx, cy, cz), f32),
            pltpu.VMEM((2, cx, cy, cz), f32),
            pltpu.VMEM((cx, cy, cz), f32),
            pltpu.VMEM((STEPS, nrec), f32),
        ),
        in_specs=[anywhere] * len(operands),
        out_specs=(vmem, vmem, vmem, vmem),
        scratch_shapes=scratch,
        compiler_params=pltpu.CompilerParams(
            collective_id=0, has_side_effects=True, vmem_limit_bytes=56 * 2**20
        ),
        name="wavefields",
    )(*operands)
    return pl.pallas_call(
        publish,
        out_shape=[jax.ShapeDtypeStruct(m.shape, m.dtype) for m in made],
        in_specs=[vmem] * len(made),
        out_specs=[vmem] * len(made),
        compiler_params=pltpu.CompilerParams(vmem_limit_bytes=4 * 2**20),
        name="publish",
    )(*made)


def solution(mesh):
    sizes = tuple(mesh.shape[axis] for axis in AXES)
    field = P(None, ("shot", "inline"), "xline", "depth")
    cell = P("inline", "xline", "depth")
    return jax.shard_map(
        functools.partial(per_device, sizes),
        mesh=mesh,
        in_specs=(
            field, field, field, field,
            cell, cell, cell, cell, cell,
            P(), P(), P("shot"), P("shot"), P("shot"), P(None, "shot"),
        ),
        out_specs=(field, field, P(("shot", "inline"), "xline", "depth"), P(None, "shot")),
        check_vma=False,
    )
```

```python
import functools

import jax
import jax.numpy as jnp
from jax import lax
from jax.experimental import pallas as pl
from jax.experimental.pallas import tpu as pltpu
from jax.sharding import PartitionSpec as P

STEPS = 4
MESH = pl.DeviceIdType.MESH
AXES = ("inline", "xline", "depth")
LANES = 128
TOP = 8

DIRECTIONS = [(a, b) for a in (-1, 0, 1) for b in (-1, 0, 1) if (a, b) != (0, 0)]
SIDES = [d for d in DIRECTIONS if d[0] == 0]
FACES = [d for d in DIRECTIONS if d[0] != 0]


def split_by(values, size):
    if size & (size - 1) == 0:
        return values >> (size.bit_length() - 1), values & (size - 1)
    quotient = lax.div(values, jnp.int32(size))
    return quotient, values - quotient * size


def two_parts(values):
    high = values.astype(jnp.bfloat16)
    return high, (values - high.astype(jnp.float32)).astype(jnp.bfloat16)


def kernel(
    sizes,
    forward_now,
    forward_before,
    adjoint_now,
    adjoint_before,
    courant,
    epsilon,
    delta,
    tilt_class,
    azimuth_class,
    tilt_given,
    azimuth_given,
    source_given,
    wavelet_given,
    cells_given,
    data_given,
    forward_out,
    adjoint_out,
    image_out,
    traces_out,
    fields,
    model,
    classes,
    factors,
    zdiff,
    zsum,
    image,
    tilt_table,
    azimuth_table,
    source_cell,
    wavelet,
    receiver_cells,
    receiver_data,
    hot_row,
    hot_lane,
    spread,
    terms,
    trace_own,
    trace_got,
    trace_all,
    load_sem,
    small_sem,
    ship_recv,
    halo_send,
    halo_recv,
    trace_recv,
    terms_recv,
    go_sem,
):
    n_in, n_x, n_d = sizes
    _, cx, cy, cz = forward_now.shape
    nrec = cells_given.shape[1]
    groups = cy // 8
    here = tuple(lax.axis_index(axis) for axis in AXES)
    rows = slice(TOP, TOP + cy)
    up = slice(TOP - 1, TOP + cy - 1)
    down = slice(TOP + 1, TOP + cy + 1)
    top = n_d - 1
    leader = here[2] == top

    def present(direction):
        ok = None
        for at, step, size in zip(here, direction, sizes):
            if step == 0:
                continue
            this = (at < size - 1) if step > 0 else (at > 0)
            ok = this if ok is None else jnp.logical_and(ok, this)
        return ok

    def target(direction, depth):
        place = {axis: at + step for axis, at, step in zip(AXES, here, direction) if step != 0}
        return {**place, "depth": depth}

    def opposite(d):
        return tuple(-step for step in d)

    live = [d for d in DIRECTIONS if all(s == 0 or n > 1 for s, n in zip(d, sizes))]
    peers = [(a, b) for a in range(n_in) for b in range(n_x) if (a, b) != (0, 0)]

    def peer(k):
        return {
            "inline": lax.rem(here[0] + peers[k][0], n_in),
            "xline": lax.rem(here[1] + peers[k][1], n_x),
        }

    def at_depth(depth):
        return {"depth": depth}

    planes, lines = pl.ds(1, cx), pl.ds(TOP, cy)
    before, now = (forward_before, adjoint_before), (forward_now, adjoint_now)

    def group_place(group, t):
        if group == "model":
            return model.at[:, :, t]
        if group == "classes":
            return classes.at[:, :, t]
        if group == "before":
            return fields.at[0, :, :, planes, t, lines]
        return fields.at[pl.ds(0, 2), group, :, planes, t, lines]

    model_copies = [(array, model, n) for n, array in enumerate((courant, epsilon, delta))]
    class_copies = [(array, classes, n) for n, array in enumerate((tilt_class, azimuth_class))]

    def members(group, t):
        if group in ("model", "classes"):
            return [
                (array, place.at[n, :, t])
                for array, place, n in (model_copies if group == "model" else class_copies)
            ]
        if group == "before":
            return [
                (before[system], fields.at[0, system, :, planes, t, lines])
                for system in range(2)
            ]
        return [
            (now[group], fields.at[1, group, :, planes, t, lines]),
            (before[group], fields.at[0, group, :, planes, t, lines]),
        ]

    def load_now(system, t):
        return pltpu.make_async_copy(
            now[system], fields.at[1, system, :, planes, t, lines], load_sem.at[system]
        )

    loaded = {"model": 2, "classes": 3, "before": 4}
    shipped = {"model": 2, "classes": 3, 0: 4, 1: 0}
    landed = {"model": 0, "classes": 1, 0: 2, 1: 3}

    def start_load(group):
        for source, place in members(group, top):
            pltpu.make_async_copy(source, place, load_sem.at[loaded[group]]).start()

    def wait_load(group):
        place = group_place(group, top)
        pltpu.make_async_copy(place, place, load_sem.at[loaded[group]]).wait()

    def ship(group, t, source, place):
        return pltpu.make_async_remote_copy(
            src_ref=source,
            dst_ref=place,
            send_sem=load_sem.at[shipped[group]],
            recv_sem=ship_recv.at[t, landed[group]],
            device_id=at_depth(top),
            device_id_type=MESH,
        )

    def start_ship(group, t):
        for source, place in members(group, t):
            ship(group, t, source, place).start()

    def whole_ship(group, t):
        place = group_place(group, t)
        return ship(group, t, place, place)

    def wait_ship(group):
        for t in range(top):
            whole_ship(group, t).wait_recv()

    smalls = [
        (cells_given, receiver_cells),
        (data_given, receiver_data),
        (tilt_given, tilt_table),
        (azimuth_given, azimuth_table),
        (source_given, source_cell),
        (wavelet_given, wavelet),
    ]

    def small(number):
        source, place = smalls[number]
        return pltpu.make_async_copy(source, place, small_sem.at[number])

    def edge(step, size, first):
        if step == 0:
            return pl.ds(first, size)
        return pl.ds(first + size - 1 if step > 0 else first, 1)

    def beyond(step, size, first):
        if step == 0:
            return pl.ds(first, size)
        return pl.ds(first - 1 if step > 0 else first + size, 1)

    def first_copy(d, system, t):
        return pltpu.make_async_remote_copy(
            src_ref=fields.at[1, system, :, edge(d[0], cx, 1), t, edge(d[1], cy, TOP)],
            dst_ref=fields.at[1, system, :, beyond(d[0], cx, 1), t, beyond(d[1], cy, TOP)],
            send_sem=halo_send.at[system, DIRECTIONS.index(d)],
            recv_sem=halo_recv.at[0, system, DIRECTIONS.index(d)],
            device_id=target(d, top),
            device_id_type=MESH,
        )

    def halo_copy(d, s, system):
        return pltpu.make_async_remote_copy(
            src_ref=fields.at[s + 1, system, :, edge(d[0], cx, 1), :, edge(d[1], cy, TOP)],
            dst_ref=fields.at[s + 1, system, :, beyond(d[0], cx, 1), :, beyond(d[1], cy, TOP)],
            send_sem=halo_send.at[system, DIRECTIONS.index(d)],
            recv_sem=halo_recv.at[s % 2, system, DIRECTIONS.index(d)],
            device_id=target(d, top),
            device_id_type=MESH,
        )

    def trace_copy(late, k):
        steps = pl.ds(STEPS - 1, 1) if late else pl.ds(0, STEPS - 1)
        return pltpu.make_async_remote_copy(
            src_ref=trace_own.at[steps],
            dst_ref=trace_got.at[k, steps],
            send_sem=small_sem.at[late],
            recv_sem=trace_recv.at[late],
            device_id=peer(k),
            device_id_type=MESH,
        )

    results = [
        (lambda t: fields.at[STEPS + 1, 0, :, pl.ds(1, cx), t, pl.ds(TOP, cy)], forward_out),
        (lambda t: fields.at[STEPS + 1, 1, :, pl.ds(1, cx), t, pl.ds(TOP, cy)], adjoint_out),
        (lambda t: image.at[t], image_out),
        (lambda t: trace_all, traces_out),
    ]

    def result_copy(number, t):
        source, place = results[number]
        return pltpu.make_async_remote_copy(
            src_ref=source(t),
            dst_ref=place,
            send_sem=load_sem.at[number],
            recv_sem=ship_recv.at[0, number],
            device_id=at_depth(t),
            device_id_type=MESH,
        )

    def give_result(number):
        for t in range(top):
            result_copy(number, t).start()

    barrier = pltpu.get_barrier_semaphore()

    def greet(place):
        pl.semaphore_signal(barrier, inc=1, device_id=place, device_id_type=MESH)

    def send_first(t, system):
        for d in sorted(live, key=lambda d: (d[0] == 0, d[1] != 0)):

            @pl.when(present(d))
            def _(d=d):
                first_copy(d, system, t).start()

    def drain_first(t, system):
        for d in live:

            @pl.when(present(d))
            def _(d=d):
                first_copy(d, system, t).wait_send()

    def clear(d):
        for s in range(STEPS):
            for system in range(2):
                place = fields.at[
                    s + 1, system, :, beyond(d[0], cx, 1), :, beyond(d[1], cy, TOP)
                ]
                place[...] = jnp.zeros(place.shape, jnp.float32)

    def clear_absent():
        for d in DIRECTIONS:
            if d not in live:
                clear(d)
            else:

                @pl.when(jnp.logical_not(present(opposite(d))))
                def _(d=d):
                    clear(d)

    def send(s, system, which):
        for d in which:
            if d in live:

                @pl.when(present(d))
                def _(d=d):
                    halo_copy(d, s, system).start()

    def receive(s, system, which):
        for d in which:
            if d in live:

                @pl.when(present(opposite(d)))
                def _(d=d):
                    halo_copy(d, s, system).wait_recv()

    def drain(s, system):
        if s == 0:
            drain_first(top, system)
            return
        for d in live:

            @pl.when(present(d))
            def _(d=d):
                halo_copy(d, s, system).wait_send()

    lane = lax.broadcasted_iota(jnp.int32, (8, LANES), 1)
    first_lane, last_lane = lane == 0, lane == LANES - 1

    def along_depth(s, system, f, plane, row):
        tiles = [fields[s + 1, system, f, plane, t, row : row + 8, :] for t in range(n_d)]
        right = [pltpu.roll(tile, 1, 1) for tile in tiles]
        left = [pltpu.roll(tile, LANES - 1, 1) for tile in tiles]
        before = [
            jnp.where(first_lane, right[t - 1] if t > 0 else 0.0, right[t]) for t in range(n_d)
        ]
        after = [
            jnp.where(last_lane, left[t + 1] if t < top else 0.0, left[t]) for t in range(n_d)
        ]
        return before, after

    def own_depth(s, system):
        for f in range(2):
            for i in range(cx):
                for r in range(groups):
                    before, after = along_depth(s, system, f, i + 1, TOP + 8 * r)
                    for t in range(n_d):
                        at = slice(TOP + 8 * r, TOP + 8 * r + 8)
                        zdiff[system, f, i + 1, t, at, :] = after[t] - before[t]
                        zsum[system, f, i, t, 8 * r : 8 * r + 8, :] = after[t] + before[t]

    def side_depth(s, system):
        for f in range(2):
            for i in range(cx):
                for row in (0, TOP + cy):
                    before, after = along_depth(s, system, f, i + 1, row)
                    for t in range(n_d):
                        zdiff[system, f, i + 1, t, row : row + 8, :] = after[t] - before[t]

    def face_depth(s, system, plane):
        for f in range(2):
            for r in range(groups):
                before, after = along_depth(s, system, f, plane, TOP + 8 * r)
                for t in range(n_d):
                    at = slice(TOP + 8 * r, TOP + 8 * r + 8)
                    zdiff[system, f, plane, t, at, :] = after[t] - before[t]

    outer = sorted({0, cx - 1})
    inner = [i for i in range(cx) if i not in outer]

    def advance(s, system, i):
        for t in range(n_d):
            axial = []
            lap = None
            doubled = []
            for f in range(2):
                now = fields.at[s + 1, system, f]
                slope = zdiff.at[system, f]
                twice = 2.0 * now[i + 1, t, rows, :]
                doubled.append(twice)
                dxx = now[i + 2, t, rows, :] + now[i, t, rows, :] - twice
                dyy = now[i + 1, t, down, :] + now[i + 1, t, up, :] - twice
                dzz = zsum[system, f, i, t] - twice
                dxy = (
                    now[i + 2, t, down, :]
                    - now[i + 2, t, up, :]
                    - now[i, t, down, :]
                    + now[i, t, up, :]
                )
                dxz = slope[i + 2, t, rows, :] - slope[i, t, rows, :]
                dyz = slope[i + 1, t, down, :] - slope[i + 1, t, up, :]
                axial.append(
                    factors[3, i, t] * dxx
                    + factors[4, i, t] * dyy
                    + factors[5, i, t] * dzz
                    + factors[6, i, t] * dxy
                    + factors[7, i, t] * dxz
                    + factors[8, i, t] * dyz
                )
                if f == 0:
                    lap = dxx + dyy + dzz
            plane_part = lap - axial[0]
            along = factors[2, i, t] * axial[1]
            if system == 0:
                row_at = lax.broadcasted_iota(jnp.int32, (cy, LANES), 0)
                lane_at = lax.broadcasted_iota(jnp.int32, (cy, LANES), 1)
                cell = (
                    (here[0] * cx + i) * (n_x * cy) + here[1] * cy + row_at
                ) * (n_d * cz) + t * cz + lane_at
                added = jnp.where(cell == source_cell[0], wavelet[s], 0.0)
            else:
                added = terms[s, i, t]
            new = []
            for f in range(2):
                value = (
                    doubled[f]
                    - fields[s, system, f, i + 1, t, rows, :]
                    + factors[f, i, t] * plane_part
                    + along
                    + added
                )
                fields[s + 2, system, f, i + 1, t, rows, :] = value
                new.append(value)
            if system == 1:
                product = (
                    fields[s + 2, 0, 0, i + 1, t, rows, :] * new[0]
                    + fields[s + 2, 0, 1, i + 1, t, rows, :] * new[1]
                )
                if s > 0:
                    product = image[t, i] + product
                if s == STEPS - 1 and t == top:
                    image_out[i] = product
                else:
                    image[t, i] = product
            if s == STEPS - 1 and t == top:
                out = forward_out if system == 0 else adjoint_out
                out[0, i] = new[0]
                out[1, i] = new[1]

    def coefficients():
        tilt_sine, tilt_cosine = jnp.sin(tilt_table[...]), jnp.cos(tilt_table[...])
        turn_sine, turn_cosine = jnp.sin(azimuth_table[...]), jnp.cos(azimuth_table[...])

        def spread_out(values):
            wide_table = jnp.zeros((8, LANES), jnp.float32)
            for k in range(values.shape[1]):
                wide_table = jnp.where(
                    lane == k, jnp.broadcast_to(values[:, k : k + 1], (8, LANES)), wide_table
                )
            return wide_table

        tilt_tables = [spread_out(v) for v in (tilt_sine, tilt_cosine)]
        turn_tables = [spread_out(v) for v in (turn_cosine, turn_sine)]

        def look(which, i, t, tables):
            found = [[] for _ in tables]
            for r in range(groups):
                chosen = classes[which, i, t, 8 * r : 8 * r + 8, :]
                for table, parts in zip(tables, found):
                    parts.append(jnp.take_along_axis(table, chosen, axis=1))
            return [jnp.concatenate(parts, axis=0) for parts in found]

        for i in range(cx):
            for t in range(n_d):
                sine, third = look(0, i, t, tilt_tables)
                turned, across = look(1, i, t, turn_tables)
                first, second = sine * turned, sine * across
                base = model[0, i, t]
                factors[0, i, t] = base * (1.0 + 2.0 * model[1, i, t])
                factors[1, i, t] = base * (1.0 + 2.0 * model[2, i, t])
                factors[2, i, t] = base
                factors[3, i, t] = first * first
                factors[4, i, t] = second * second
                factors[5, i, t] = third * third
                factors[6, i, t] = 0.5 * first * second
                factors[7, i, t] = 0.5 * first * third
                factors[8, i, t] = 0.5 * second * third

    volume = cx * cy
    wide = n_d * cz

    def receivers():
        cells = receiver_cells[...]
        upper, depth_at = split_by(cells, wide)
        inline_at, xline_at = split_by(upper, n_x * cy)
        inline_at = inline_at - here[0] * cx
        xline_at = xline_at - here[1] * cy
        inside = (inline_at >= 0) & (inline_at < cx) & (xline_at >= 0) & (xline_at < cy)
        row_of = jnp.where(inside, inline_at * cy + xline_at, -1)
        for start in range(0, volume, 16):
            row_at = start + lax.broadcasted_iota(jnp.int32, (16, nrec), 0)
            match = row_at == jnp.broadcast_to(row_of, (16, nrec))
            hot_row[start : start + 16, :] = jnp.where(match, 1.0, 0.0)
        for start in range(0, wide, 16):
            lane_at = start + lax.broadcasted_iota(jnp.int32, (16, nrec), 0)
            match = lane_at == jnp.broadcast_to(depth_at, (16, nrec))
            hot_lane[start : start + 16, :] = jnp.where(match, 1.0, 0.0).astype(jnp.bfloat16)

    def injection(s):
        for number, part in enumerate(two_parts(receiver_data[s : s + 1, :])):
            spread[number * volume : (number + 1) * volume, :] = hot_row[...].astype(
                jnp.bfloat16
            ) * jnp.broadcast_to(part, (volume, nrec))
        got = lax.dot_general(
            spread[...],
            hot_lane[...],
            (((1,), (1,)), ((), ())),
            preferred_element_type=jnp.float32,
        )
        total = got[:volume] + got[volume:]
        for i in range(cx):
            for t in range(n_d):
                terms[s, i, t] = total[i * cy : (i + 1) * cy, t * cz : (t + 1) * cz]

    def sample(s):
        tiles = [
            jnp.concatenate(
                [fields[s + 2, 0, 0, i + 1, t, rows, :] for i in range(cx)], axis=0
            )
            for t in range(n_d)
        ]
        split = [two_parts(tile) for tile in tiles]
        parts = jnp.concatenate(
            [
                jnp.concatenate([split[t][part] for t in range(n_d)], axis=1)
                for part in range(2)
            ],
            axis=0,
        )
        picked = jnp.dot(parts, hot_lane[...], preferred_element_type=jnp.float32)
        picked = picked[:volume] + picked[volume:]
        trace_own[s] = jnp.sum(picked * hot_row[...], axis=0, keepdims=True)

    def share(late):
        for k in range(len(peers)):
            trace_copy(late, k).start()

    def whole_trace(late):
        steps = pl.ds(STEPS - 1, 1) if late else pl.ds(0, STEPS - 1)
        place = trace_got.at[pl.ds(0, len(peers)), steps]
        return pltpu.make_async_remote_copy(
            src_ref=place,
            dst_ref=place,
            send_sem=small_sem.at[late],
            recv_sem=trace_recv.at[late],
            device_id=peer(0),
            device_id_type=MESH,
        )

    def finish_trace(late):
        if peers:
            whole_trace(late).wait_recv()
        for s in [STEPS - 1] if late else range(STEPS - 1):
            total = trace_own[s]
            for k in range(len(peers)):
                total = total + trace_got[k, s]
            traces_out[s : s + 1, :] = total
            trace_all[s : s + 1, :] = total

    def terms_copy(first, count):
        return pltpu.make_async_remote_copy(
            src_ref=terms.at[pl.ds(first, count)],
            dst_ref=terms.at[pl.ds(first, count)],
            send_sem=small_sem.at[2],
            recv_sem=terms_recv.at[min(first, 1)],
            device_id=at_depth(top),
            device_id_type=MESH,
        )

    nearby = max(n_in, n_x) <= STEPS
    neighbours = jnp.int32(0)
    for d in live:
        neighbours = neighbours + jnp.where(present(d), 1, 0)

    @pl.when(jnp.logical_not(leader))
    def _():
        greet(at_depth(top))
        for system in range(2):
            load_now(system, here[2]).start()
        for number in (0, 1):
            small(number).start()
        pl.semaphore_wait(barrier, 1)
        for group in ("classes", "model"):
            start_ship(group, here[2])
        for system in range(2):
            load_now(system, here[2]).wait()
        pl.semaphore_wait(go_sem, 1)
        for system in range(2):
            send_first(here[2], system)
            start_ship(system, here[2])
        for number in (0, 1):
            small(number).wait()

        @pl.when(here[2] == 0)
        def _():
            receivers()
            for s in range(STEPS):
                injection(s)
                terms_copy(s, 1).start()
            terms_copy(0, STEPS).wait_send()

        for group in ("classes", "model", 0, 1):
            whole_ship(group, here[2]).wait_send()
        for system in range(2):
            drain_first(here[2], system)
        for number in range(len(results)):
            result_copy(number, here[2]).wait_recv()

    @pl.when(leader)
    def _():
        if nearby:
            for d in sorted(live, key=lambda d: d[0] * d[1] != 0):

                @pl.when(present(d))
                def _(d=d):
                    greet(target(d, top))

        else:
            for k in range(len(peers)):
                greet(peer(k))
        for t in range(top):
            greet(at_depth(t))
        for system in range(2):
            load_now(system, top).start()
        for number in range(len(smalls)):
            small(number).start()
        for group in ("classes", "model", "before"):
            start_load(group)
        pl.semaphore_wait(barrier, (neighbours if nearby else len(peers)) + top)
        for t in range(top):
            pl.semaphore_signal(
                go_sem, inc=1, device_id=at_depth(t), device_id_type=MESH
            )
        for system in range(2):
            load_now(system, top).wait()
            send_first(top, system)
        clear_absent()
        for number in range(len(smalls)):
            small(number).wait()
        for group in ("classes", "model"):
            wait_load(group)
            wait_ship(group)
        coefficients()
        receivers()
        wait_load("before")
        wait_ship(0)
        own_depth(0, 0)
        if top == 0:
            for s in range(STEPS):
                injection(s)
        for s in range(STEPS):
            for system in range(2):
                if s == 0 and system == 1:
                    wait_ship(1)
                    own_depth(0, 1)
                if system == 1 and top > 0 and s < 2:
                    terms_copy(s, STEPS - 1 if s else 1).wait_recv()
                drain(s, system)
                receive(s, system, SIDES)
                side_depth(s, system)
                for i in inner:
                    advance(s, system, i)
                if cx > 1:
                    for i, side in ((0, 1), (cx - 1, -1)):
                        receive(s, system, [d for d in FACES if d[0] == side])
                        face_depth(s, system, 0 if side > 0 else cx + 1)
                        advance(s, system, i)
                        if s < STEPS - 1:
                            send(s + 1, system, [d for d in FACES if d[0] == -side])
                else:
                    receive(s, system, FACES)
                    for plane in (0, cx + 1):
                        face_depth(s, system, plane)
                    advance(s, system, 0)
                    if s < STEPS - 1:
                        send(s + 1, system, FACES)
                if s < STEPS - 1:
                    send(s + 1, system, SIDES)
                    own_depth(s + 1, system)
                if s == STEPS - 1:
                    if system == 0:
                        sample(s)
                        share(1)
                elif system == 1:
                    sample(s)
                    if s == STEPS - 2:
                        share(0)
                if s == STEPS - 1:
                    give_result(system)
        give_result(2)
        for late in range(2):
            finish_trace(late)
        give_result(3)
        if peers:
            for late in range(2):
                whole_trace(late).wait_send()
        for number in range(len(results)):
            for t in range(top):
                result_copy(number, t).wait_send()


def publish(*refs):
    half = len(refs) // 2
    for source, place in zip(refs[:half], refs[half:]):
        place[...] = source[...]


def per_device(sizes, *operands):
    shapes = [operand.shape for operand in operands]
    _, cx, cy, cz = shapes[0]
    nrec = shapes[13][0]
    n_in, n_x, n_d = sizes
    operands = list(operands)
    for which in (9, 10, 13):
        operands[which] = operands[which].reshape(1, -1)
    f32, bf16 = jnp.float32, jnp.bfloat16
    padded = cy + 2 * TOP
    chips = n_in * n_x
    count = len(DIRECTIONS)
    others = max(n_d - 1, 1)
    dma = pltpu.SemaphoreType.DMA
    scratch = [
        pltpu.VMEM((STEPS + 2, 2, 2, cx + 2, n_d, padded, cz), f32),
        pltpu.VMEM((3, cx, n_d, cy, cz), f32),
        pltpu.VMEM((2, cx, n_d, cy, cz), jnp.int32),
        pltpu.VMEM((9, cx, n_d, cy, cz), f32),
        pltpu.VMEM((2, 2, cx + 2, n_d, padded, cz), f32),
        pltpu.VMEM((2, 2, cx, n_d, cy, cz), f32),
        pltpu.VMEM((n_d, cx, cy, cz), f32),
        pltpu.VMEM(operands[9].shape, f32),
        pltpu.VMEM(operands[10].shape, f32),
        pltpu.SMEM(shapes[11], jnp.int32),
        pltpu.SMEM(shapes[12], f32),
        pltpu.VMEM(operands[13].shape, jnp.int32),
        pltpu.VMEM(shapes[14], f32),
        pltpu.VMEM((cx * cy, nrec), f32),
        pltpu.VMEM((n_d * cz, nrec), bf16),
        pltpu.VMEM((2 * cx * cy, nrec), bf16),
        pltpu.VMEM((STEPS, cx, n_d, cy, cz), f32),
        pltpu.VMEM((STEPS, 1, nrec), f32),
        pltpu.VMEM((chips, STEPS, 1, nrec), f32),
        pltpu.VMEM((STEPS, nrec), f32),
        dma((5,)),
        dma((6,)),
        dma((others, 4)),
        dma((2, count)),
        dma((2, 2, count)),
        dma((2,)),
        dma((2,)),
        pltpu.SemaphoreType.REGULAR,
    ]
    vmem = pl.BlockSpec(memory_space=pltpu.VMEM)
    anywhere = pl.BlockSpec(memory_space=pl.ANY)
    made = pl.pallas_call(
        functools.partial(kernel, sizes),
        out_shape=(
            pltpu.VMEM((2, cx, cy, cz), f32),
            pltpu.VMEM((2, cx, cy, cz), f32),
            pltpu.VMEM((cx, cy, cz), f32),
            pltpu.VMEM((STEPS, nrec), f32),
        ),
        in_specs=[anywhere] * len(operands),
        out_specs=(vmem, vmem, vmem, vmem),
        scratch_shapes=scratch,
        compiler_params=pltpu.CompilerParams(
            collective_id=0, has_side_effects=True, vmem_limit_bytes=56 * 2**20
        ),
        name="wavefields",
    )(*operands)
    return pl.pallas_call(
        publish,
        out_shape=[jax.ShapeDtypeStruct(m.shape, m.dtype) for m in made],
        in_specs=[vmem] * len(made),
        out_specs=[vmem] * len(made),
        compiler_params=pltpu.CompilerParams(vmem_limit_bytes=4 * 2**20),
        name="publish",
    )(*made)


def solution(mesh):
    sizes = tuple(mesh.shape[axis] for axis in AXES)
    field = P(None, ("shot", "inline"), "xline", "depth")
    cell = P("inline", "xline", "depth")
    return jax.shard_map(
        functools.partial(per_device, sizes),
        mesh=mesh,
        in_specs=(
            field, field, field, field,
            cell, cell, cell, cell, cell,
            P(), P(), P("shot"), P("shot"), P("shot"), P(None, "shot"),
        ),
        out_specs=(field, field, P(("shot", "inline"), "xline", "depth"), P(None, "shot")),
        check_vma=False,
    )
```
